128 devices in a mesh: section: 8 (over y, z_lo), seq: 2 (over core), tensor: 8 (over z_hi, x).
Axes of the slice: x: 4, y: 4, z: 4 (z_hi: 2, z_lo: 2; z = z_hi * 2 + z_lo), core: 2. Of those that a mesh axis runs over, the one named last changes fastest.
Arguments:
- states_in: bfloat16 [1, 256, 4608], P(None, 'seq', 'tensor'), may hold values from -100 to 100
- span_order: int32 [4], replicated, may hold values from 0 to 3, each once
- pre_gain: bfloat16 [8, 4608], P('section'), may hold values from 0.25 to 1.75
- w_query: bfloat16 [8, 4608, 4096], P('section', None, 'tensor'), may hold values from -0.09375 to 0.09375
- w_key: bfloat16 [8, 4608, 2048], P('section', None, 'tensor'), may hold values from -0.09375 to 0.09375
- w_value: bfloat16 [8, 4608, 2048], P('section', None, 'tensor'), may hold values from -0.09375 to 0.09375
- w_out: bfloat16 [8, 4096, 4608], P('section', 'tensor'), may hold values from -0.125 to 0.125
- post_gain: bfloat16 [8, 4608], P('section'), may hold values from 0.25 to 1.75
Outputs:
- states: bfloat16 [8, 1, 256, 4608], P('section', None, 'seq', 'tensor')
The draws below stay inside these ranges and needn't reach their ends.
Inputs may be any that keep to these rules, and one draw needn't show every extreme that they name: Each span number appears once; row block j of 64 rows holds the tokens from position span_order[j] * 64 on.
All inputs are finite; a program needn't handle non-finite values.
Results may differ from the reference program's by a relative error of at most 0.024.
Values may be sent and summed in bfloat16 or wider, within the bound.
No kernel may reach another device: no remote copies, remote signals or barrier semaphores. Data moves between devices by JAX's collectives and lax.ppermute only.
A program may use at most 64 MiB of HBM per device.

```python
import jax
import jax.numpy as jnp
from jax import lax

D = 4608
HEADS = 32
KV_HEADS = 16
HEAD_DIM = 128
MICRO = 1
LAYERS = 8
SEQLEN = 256
SPAN = 64
N_SEQ = 2
N_TENSOR = 8


def draw_states_in(key, part):
    shape_full = (MICRO, SEQLEN, D)
    key_base = jax.random.fold_in(key, 11)
    sample = jnp.clip(jax.random.normal(key_base, shape_full, jnp.float32), -4.0, 4.0)
    return sample.astype(jnp.bfloat16)


def spiked(entries, own_key, source, target, blocks, factor):
    owner, partner = [(jnp.arange(entries.shape[axis_at]) // (entries.shape[axis_at] // blocks)).reshape([-1 if axis == axis_at else 1 for axis in range(entries.ndim)]) for axis_at in (source, target)]
    chosen = jax.random.permutation(own_key, blocks)[partner]
    strong = (owner == chosen) | (owner == (partner + blocks // 2) % blocks)
    return jnp.where(strong, factor * entries, entries)


def level_of(rng, shape, cuts, low, high):
    def one(axis_at, shards_of):
        draws = jax.random.uniform(jax.random.fold_in(jax.random.fold_in(rng, 6), axis_at), (shards_of,), jnp.float32, low / len(cuts), high / len(cuts))
        return jnp.repeat(jnp.exp(draws), shape[axis_at] // shards_of).reshape((-1,) + (1,) * (len(shape) - axis_at - 1))

    factor_of = one(*cuts[0])
    for cut in cuts[1:]:
        factor_of = factor_of * one(*cut)
    return factor_of


def gaussian(stream_key, extent, deviation, reach, cuts=(), held_as=jnp.bfloat16):
    entries = jax.random.normal(stream_key, extent, jnp.float32) * deviation
    if len(cuts) > 0:
        entries = level_of(stream_key, extent, cuts, -0.22, 0.18) * entries
    return jnp.clip(entries, min=-reach, max=reach).astype(held_as)


def gaussian_with(rng, dims, deviation, reach, cuts, heavy, held_as=jnp.bfloat16):
    values = deviation * jax.random.normal(rng, dims, jnp.float32)
    if cuts:
        values = values * level_of(rng, dims, cuts, -0.22, 0.18)
    return jnp.clip(spiked(values, jax.random.fold_in(rng, 3), *heavy), -reach, reach).astype(held_as)


def setup_inputs(seed: int = 0) -> dict:
    splits = jax.random.split(jax.random.key(seed), 9)
    states_in = draw_states_in(jax.random.fold_in(splits[8], 71), 0)
    span_order = jax.random.permutation(splits[1], 2 * N_SEQ).astype(jnp.int32)
    pre_gain = jnp.clip(1.0 + 0.15 * jax.random.normal(splits[2], (LAYERS, D), jnp.float32), 0.25, 1.75).astype(jnp.bfloat16)
    w_query = gaussian(splits[3], (LAYERS, D, HEADS * HEAD_DIM), D ** -0.5, 0.09375, ((0, 8), (2, 8)))
    w_key = gaussian(splits[4], (LAYERS, D, KV_HEADS * HEAD_DIM), D ** -0.5, 0.09375, ((0, 8), (2, 8)))
    w_value = gaussian(splits[5], (LAYERS, D, KV_HEADS * HEAD_DIM), D ** -0.5, 0.09375, ((0, 8), (2, 8)))
    w_out = gaussian_with(splits[6], (LAYERS, HEADS * HEAD_DIM, D), (HEADS * HEAD_DIM) ** -0.5, 0.125, ((0, 8), (1, 8)), (1, 2, 8, 2.0))
    post_gain = jnp.clip(1.0 + 0.15 * jax.random.normal(splits[7], (LAYERS, D), jnp.float32), 0.25, 1.75).astype(jnp.bfloat16)
    return {"states_in": states_in, "span_order": span_order, "pre_gain": pre_gain, "w_query": w_query, "w_key": w_key, "w_value": w_value, "w_out": w_out, "post_gain": post_gain}


softcap_limit = 50.0
query_scale = 144.0 ** (-0.5)
epsilon = 1e-06
rotary_base = 10000.0

def rounded(array):
    return lax.optimization_barrier(array.astype(jnp.bfloat16)).astype(jnp.float32)

def rotate(vectors, places):
    half_dim = vectors.shape[-1] // 2
    inverse = rotary_base ** (-(jnp.arange(half_dim, dtype=jnp.float32) * 2.0 / vectors.shape[-1]))
    angles = places.astype(jnp.float32)[:, None] * inverse[None, :]
    cos_part = jnp.cos(angles)[:, None, :]
    sin_part = jnp.sin(angles)[:, None, :]
    lower_half = vectors[..., :half_dim]
    upper_half = vectors[..., half_dim:]
    return jnp.concatenate([lower_half * cos_part - upper_half * sin_part, upper_half * cos_part + lower_half * sin_part], axis=-1)

def one_layer(stream_in, places, allowed, gain_in, query_w, key_w, value_w, out_w, gain_out):
    group_size = HEADS // KV_HEADS
    local_heads = HEADS // N_TENSOR
    stream = stream_in.astype(jnp.float32)
    normed = (stream * lax.rsqrt(lax.optimization_barrier(jnp.mean(stream * stream, axis=1, keepdims=True)) + epsilon) * gain_in.astype(jnp.float32)).astype(jnp.bfloat16)
    queries = jnp.dot(normed, query_w, preferred_element_type=jnp.float32).reshape(SEQLEN, HEADS, HEAD_DIM)
    queries = rounded(rotate(queries, places) * query_scale).reshape(SEQLEN, KV_HEADS, group_size, HEAD_DIM)
    key_rows = jnp.dot(normed, key_w, preferred_element_type=jnp.float32).reshape(SEQLEN, KV_HEADS, HEAD_DIM)
    key_rows = rounded(rotate(key_rows, places))
    values = rounded(jnp.dot(normed, value_w, preferred_element_type=jnp.float32)).reshape(SEQLEN, KV_HEADS, HEAD_DIM)
    scores = jnp.einsum('tkgd,pkd->kgtp', queries, key_rows, precision=lax.Precision.HIGHEST)
    capped = softcap_limit * jnp.tanh(scores / softcap_limit)
    weight = jnp.where(allowed[None, None], jnp.exp(capped), jnp.float32(0.0))
    totals = lax.optimization_barrier(jnp.sum(weight, axis=3))
    numerator = jnp.einsum('kgtp,pkd->tkgd', rounded(weight), values, precision=lax.Precision.HIGHEST)
    attended = (numerator / jnp.transpose(totals, (2, 0, 1))[..., None]).astype(jnp.bfloat16)
    attended = attended.reshape(SEQLEN, N_TENSOR, local_heads * HEAD_DIM)
    out_groups = out_w.reshape(N_TENSOR, local_heads * HEAD_DIM, D)
    projected = jnp.zeros((SEQLEN, D), jnp.float32)
    for group_index in range(N_TENSOR):
        term = jnp.dot(attended[:, group_index], out_groups[group_index], preferred_element_type=jnp.float32)
        projected = projected + rounded(term)
    scaling = lax.rsqrt(lax.optimization_barrier(jnp.mean(projected * projected, axis=1, keepdims=True)) + epsilon)
    return (stream + projected * scaling * gain_out.astype(jnp.float32)).astype(jnp.bfloat16)

def reference(states_in, span_order, pre_gain, w_query, w_key, w_value, w_out, post_gain):
    row_ids = jnp.arange(SEQLEN, dtype=jnp.int32)
    places = (span_order[row_ids // SPAN] * SPAN + row_ids % SPAN).astype(jnp.int32)
    allowed = places[None, :] <= places[:, None]
    per_layer = []
    for layer_index in range(LAYERS):
        per_layer.append([])
    for micro_index in range(MICRO):
        stream = states_in[micro_index]
        for layer_index in range(LAYERS):
            stream = one_layer(stream, places, allowed, pre_gain[layer_index], w_query[layer_index], w_key[layer_index], w_value[layer_index], w_out[layer_index], post_gain[layer_index])
            per_layer[layer_index].append(stream)
    return jnp.stack([jnp.stack(items, axis=0) for items in per_layer], axis=0)
```

```python
import jax
import jax.numpy as jnp
from jax import lax
from jax.sharding import PartitionSpec as P

HEAD_DIM = 128
CHUNKS = 2

softcap_limit = 50.0
query_scale = 144.0 ** (-0.5)
epsilon = 1e-06
rotary_base = 10000.0
f32 = jnp.float32
bf16 = jnp.bfloat16


def rotate(vectors, cos_part, sin_part):
    half_dim = vectors.shape[-1] // 2
    lower_half = vectors[..., :half_dim]
    upper_half = vectors[..., half_dim:]
    return jnp.concatenate(
        [
            lower_half * cos_part - upper_half * sin_part,
            upper_half * cos_part + lower_half * sin_part,
        ],
        axis=-1,
    )


def exchange(pieces):
    return lax.all_to_all(pieces, "tensor", split_axis=0, concat_axis=0, tiled=True)


def spread(x, size):
    return exchange(jnp.broadcast_to(x[None], (size, *x.shape)))


def body(states_in, span_order, pre_gain, w_query, w_key, w_value, w_out, post_gain):
    _, row_count, width_part = states_in.shape
    width = pre_gain.shape[1]
    q_width = w_query.shape[2]
    kv_width = w_key.shape[2]
    kv_heads = kv_width // HEAD_DIM
    group = q_width // kv_width
    sections = lax.axis_size("section")
    tensors = lax.axis_size("tensor")
    section_rank = lax.axis_index("section")
    seq_rank = lax.axis_index("seq")
    tensor_rank = lax.axis_index("tensor")
    seqs = lax.axis_size("seq")
    spans = span_order.shape[0]
    rows = row_count // CHUNKS
    own = rows // tensors
    chunk_len = rows * seqs
    total_len = chunk_len * CHUNKS
    gain_in = pre_gain[0].astype(f32)
    gain_out = post_gain[0].astype(f32)
    ids = jnp.arange(spans, dtype=jnp.int32)

    blocks = lax.all_gather(states_in[0], "seq", axis=0).reshape(spans, rows, width_part)
    block_of = jnp.sum(jnp.where(span_order[None, :] == ids[:, None], ids[None, :], 0), axis=1)
    picked = jnp.stack(
        [
            lax.dynamic_index_in_dim(
                blocks,
                lax.dynamic_index_in_dim(block_of, c * seqs + seq_rank, 0, keepdims=False),
                0,
                keepdims=False,
            )
            for c in range(CHUNKS)
        ]
    )
    first_rows = spread(picked, tensors)
    first_rows = jnp.moveaxis(first_rows, 0, 2).reshape(CHUNKS, rows, width)

    places = (
        jnp.arange(CHUNKS, dtype=jnp.int32)[:, None] * chunk_len
        + seq_rank * rows
        + jnp.arange(rows, dtype=jnp.int32)[None, :]
    )
    half = HEAD_DIM // 2
    inverse = rotary_base ** (-(jnp.arange(half, dtype=f32) * 2.0 / HEAD_DIM))
    angles = places.astype(f32)[..., None] * inverse
    cos_all, sin_all = (jnp.cos(angles), jnp.sin(angles))

    def layer(full, slot, keys, values_held):
        stream = full.astype(f32)
        normed = (
            stream * lax.rsqrt(jnp.mean(stream * stream, axis=1, keepdims=True) + epsilon) * gain_in
        ).astype(bf16)
        cos_part = lax.dynamic_index_in_dim(cos_all, slot, 0, keepdims=False)[:, None, :]
        sin_part = lax.dynamic_index_in_dim(sin_all, slot, 0, keepdims=False)[:, None, :]
        queries = jnp.dot(normed, w_query[0], preferred_element_type=f32)
        queries = rotate(queries.reshape(rows, -1, HEAD_DIM), cos_part, sin_part) * query_scale
        queries = queries.astype(bf16).reshape(rows, kv_heads, group, HEAD_DIM)
        key_rows = jnp.dot(normed, w_key[0], preferred_element_type=f32)
        key_rows = rotate(key_rows.reshape(rows, -1, HEAD_DIM), cos_part, sin_part)
        key_rows = key_rows.astype(bf16).reshape(rows, kv_width)
        value_rows = jnp.dot(normed, w_value[0], preferred_element_type=f32).astype(bf16)
        both = lax.all_gather(jnp.concatenate([key_rows, value_rows], axis=1), "seq", axis=0)
        both = both.reshape(chunk_len, 2 * kv_width)
        keys = lax.dynamic_update_slice_in_dim(keys, both[:, :kv_width], slot * chunk_len, 0)
        values_held = lax.dynamic_update_slice_in_dim(
            values_held, both[:, kv_width:], slot * chunk_len, 0
        )
        scores = jnp.einsum(
            "tkgd,pkd->kgtp",
            queries,
            keys.reshape(total_len, kv_heads, HEAD_DIM),
            preferred_element_type=f32,
        )
        capped = softcap_limit * jnp.tanh(scores / softcap_limit)
        my_places = lax.dynamic_index_in_dim(places, slot, 0, keepdims=False)
        allowed = jnp.arange(total_len, dtype=jnp.int32)[None, :] <= my_places[:, None]
        weight = jnp.where(allowed[None, None], jnp.exp(capped), f32(0.0))
        totals = jnp.sum(weight, axis=3)
        numerator = jnp.einsum(
            "kgtp,pkd->tkgd",
            weight.astype(bf16),
            values_held.reshape(total_len, kv_heads, HEAD_DIM),
            preferred_element_type=f32,
        )
        attended = (numerator / jnp.transpose(totals, (2, 0, 1))[..., None]).astype(bf16)
        partial_value = jnp.dot(
            attended.reshape(rows, q_width), w_out[0], preferred_element_type=f32
        ).astype(bf16)
        arrived = exchange(partial_value.reshape(tensors, own, width))
        projected = arrived.astype(f32).sum(axis=0)
        scaling = lax.rsqrt(jnp.mean(projected * projected, axis=1, keepdims=True) + epsilon)
        held = lax.dynamic_slice_in_dim(full, tensor_rank * own, own, 0).astype(f32)
        return (held + projected * scaling * gain_out).astype(bf16), keys, values_held

    def work(carried, tick_index):
        full, keys, values_held, record = carried
        slot_index = tick_index - section_rank
        slot = jnp.clip(slot_index, 0, CHUNKS - 1)
        new_rows, keys, values_held = layer(full, slot, keys, values_held)
        is_valid = slot_index == slot
        placed = lax.dynamic_update_index_in_dim(record, new_rows, slot, 0)
        record = jnp.where(is_valid, placed, record)
        return new_rows, keys, values_held, record

    def tick(carried, tick_index):
        new_rows, keys, values_held, record = work(carried, tick_index)
        moved = lax.ppermute(new_rows, "section", [(i, i + 1) for i in range(sections - 1)])
        full = spread(moved, tensors).reshape(rows, width)
        following = lax.dynamic_index_in_dim(
            first_rows, jnp.minimum(tick_index + 1, CHUNKS - 1), 0, keepdims=False
        )
        full = jnp.where(section_rank == 0, following, full)
        return (full, keys, values_held, record), None

    tick_total = sections + CHUNKS - 1
    start = (
        first_rows[0],
        jnp.zeros((total_len, kv_width), bf16),
        jnp.zeros((total_len, kv_width), bf16),
        jnp.zeros((CHUNKS, own, width), bf16),
    )
    carried, _ = lax.scan(tick, start, jnp.arange(tick_total - 1, dtype=jnp.int32))
    record = work(carried, jnp.int32(tick_total - 1))[3]

    pieces = record.reshape(CHUNKS, own, tensors, width_part)
    pieces = exchange(jnp.moveaxis(pieces, 2, 0))
    pieces = jnp.moveaxis(pieces, 0, 1).reshape(CHUNKS, rows, width_part)
    ordered = lax.all_gather(pieces, "seq", axis=1).reshape(spans, rows, width_part)
    mine = lax.dynamic_slice_in_dim(span_order, seq_rank * CHUNKS, CHUNKS, 0)
    out = [lax.dynamic_index_in_dim(ordered, mine[j], 0, keepdims=False) for j in range(CHUNKS)]
    return jnp.concatenate(out, axis=0)[None, None]


def solution(mesh):
    in_specs = (
        P(None, "seq", "tensor"),
        P(),
        P("section", None),
        P("section", None, "tensor"),
        P("section", None, "tensor"),
        P("section", None, "tensor"),
        P("section", "tensor", None),
        P("section", None),
    )
    out_specs = P("section", None, "seq", "tensor")
    return jax.shard_map(body, mesh=mesh, in_specs=in_specs, out_specs=out_specs, check_vma=False)
```

```python
import jax
import jax.numpy as jnp
from jax import lax
from jax.experimental import pallas as pl
from jax.experimental.pallas import tpu as pltpu
from jax.sharding import PartitionSpec as P

HEAD_DIM = 128
CHUNKS = 2

softcap_limit = 50.0
query_scale = 144.0 ** (-0.5)
epsilon = 1e-06
rotary_base = 10000.0
f32 = jnp.float32
bf16 = jnp.bfloat16

VMEM = pl.BlockSpec(memory_space=pltpu.VMEM)
SMEM = pl.BlockSpec(memory_space=pltpu.SMEM)
HBM = pl.BlockSpec(memory_space=pl.ANY)


def exchange(pieces):
    return lax.all_to_all(pieces, "tensor", split_axis=0, concat_axis=0, tiled=True)


def rope(u, cos_full, sin_full):
    return u * cos_full + pltpu.roll(u, HEAD_DIM // 2, 1) * sin_full


def key_value_kernel(place_ref, x_ref, gain_ref, cos_ref, sin_ref, wk_ref, wv_ref,
                     kv_ref, normed_ref, wk_buf, wv_buf, sems):
    steps, block, kv_width = wk_buf.shape
    rows, width = normed_ref.shape

    def copies(k):
        at = pl.ds(k * block, block)
        return (
            pltpu.make_async_copy(wk_ref.at[0, at], wk_buf.at[k], sems.at[0, k]),
            pltpu.make_async_copy(wv_ref.at[0, at], wv_buf.at[k], sems.at[1, k]),
        )

    for k in range(steps):
        for copy in copies(k):
            copy.start()
    squares = jnp.zeros((rows, 1), f32)
    for k in range(steps):
        x = x_ref[:, :, k * block:(k + 1) * block].astype(f32).reshape(rows, block)
        squares += jnp.sum(x * x, axis=1, keepdims=True)
    scaling = lax.rsqrt(squares / width + epsilon)
    for k in range(steps):
        at = slice(k * block, (k + 1) * block)
        x = x_ref[:, :, at].astype(f32).reshape(rows, block)
        normed_ref[:, at] = (x * scaling * gain_ref[:, at].astype(f32)).astype(bf16)
    key_sum = jnp.zeros((rows, kv_width), f32)
    value_sum = jnp.zeros((rows, kv_width), f32)
    for k in range(steps):
        for copy in copies(k):
            copy.wait()
        part = normed_ref[:, k * block:(k + 1) * block]
        key_sum += jnp.dot(part, wk_buf[k], preferred_element_type=f32)
        value_sum += jnp.dot(part, wv_buf[k], preferred_element_type=f32)
    slot = place_ref[0]
    cos_full, sin_full = cos_ref[slot], sin_ref[slot]
    for head in range(kv_width // HEAD_DIM):
        at = slice(head * HEAD_DIM, (head + 1) * HEAD_DIM)
        kv_ref[:, at] = rope(key_sum[:, at], cos_full, sin_full).astype(bf16)
    kv_ref[:, kv_width:] = value_sum.astype(bf16)


def query_kernel(place_ref, normed_ref, cos_ref, sin_ref, wq_ref, q_ref, wq_buf, sems):
    steps, block, q_width = wq_buf.shape
    rows = normed_ref.shape[0]

    def copy(k):
        return pltpu.make_async_copy(wq_ref.at[0, pl.ds(k * block, block)], wq_buf.at[k], sems.at[k])

    for k in range(steps):
        copy(k).start()
    total = jnp.zeros((rows, q_width), f32)
    for k in range(steps):
        copy(k).wait()
        total += jnp.dot(
            normed_ref[:, k * block:(k + 1) * block], wq_buf[k], preferred_element_type=f32
        )
    slot = place_ref[0]
    cos_full, sin_full = cos_ref[slot], sin_ref[slot]
    for head in range(q_width // HEAD_DIM):
        at = slice(head * HEAD_DIM, (head + 1) * HEAD_DIM)
        q_ref[:, at] = (rope(total[:, at], cos_full, sin_full) * query_scale).astype(bf16)


def attention_kernel(place_ref, q_ref, own_ref, other_ref, past_own_ref, past_other_ref, wo_ref,
                     out_ref, attended_ref, wo_buf, sems):
    steps, _, block = wo_buf.shape
    rows, q_width = q_ref.shape
    kv_width = own_ref.shape[1] // 2
    kv_heads = kv_width // HEAD_DIM
    group = q_width // kv_width

    def copy(n):
        return pltpu.make_async_copy(wo_ref.at[0, :, pl.ds(n * block, block)], wo_buf.at[n], sems.at[n])

    for n in range(steps):
        copy(n).start()
    has_past = place_ref[0] > 0
    is_later = place_ref[1] > 0
    row = lax.broadcasted_iota(jnp.int32, (group * rows, 4 * rows), 0) % rows
    col = lax.broadcasted_iota(jnp.int32, (group * rows, 4 * rows), 1)
    other_to = jnp.where(is_later, 2 * rows, rows)
    past_to = jnp.where(has_past, 4 * rows, 2 * rows)
    allowed = (
        ((col < rows) & (col <= row))
        | ((col >= rows) & (col < other_to))
        | ((col >= 2 * rows) & (col < past_to))
    )
    sources = (own_ref, other_ref, past_own_ref, past_other_ref)
    for head in range(kv_heads):
        at = slice(head * HEAD_DIM, (head + 1) * HEAD_DIM)
        value_at = slice(kv_width + head * HEAD_DIM, kv_width + (head + 1) * HEAD_DIM)
        keys = jnp.concatenate([s[:, at] for s in sources], axis=0)
        values = jnp.concatenate([s[:, value_at] for s in sources], axis=0)
        first = head * group * HEAD_DIM
        queries = jnp.concatenate(
            [q_ref[:, first + g * HEAD_DIM:first + (g + 1) * HEAD_DIM] for g in range(group)], axis=0
        )
        scores = lax.dot_general(
            queries, keys, (((1,), (1,)), ((), ())), preferred_element_type=f32
        )
        capped = softcap_limit * jnp.tanh(scores / softcap_limit)
        weight = jnp.where(allowed, jnp.exp(capped), f32(0.0))
        totals = jnp.sum(weight, axis=1, keepdims=True)
        numerator = jnp.dot(weight.astype(bf16), values, preferred_element_type=f32)
        attended = (numerator / totals).astype(bf16)
        for g in range(group):
            attended_ref[:, first + g * HEAD_DIM:first + (g + 1) * HEAD_DIM] = attended[
                g * rows:(g + 1) * rows
            ]
    owners, own = out_ref.shape[:2]
    for n in range(steps):
        copy(n).wait()
        part = jnp.dot(attended_ref[...], wo_buf[n], preferred_element_type=f32)
        out_ref[:, :, n * block:(n + 1) * block] = part.reshape(owners, own, block).astype(bf16)


def combine_kernel(arrived_ref, held_ref, gain_ref, out_ref):
    width = out_ref.shape[1]
    projected = jnp.sum(arrived_ref[...].astype(f32), axis=0)
    mean = jnp.sum(projected * projected, axis=1, keepdims=True) / width
    scaled = projected * lax.rsqrt(mean + epsilon) * gain_ref[...].astype(f32)
    out_ref[...] = (held_ref[...].astype(f32) + scaled).astype(bf16)


def body(states_in, span_order, pre_gain, w_query, w_key, w_value, w_out, post_gain):
    _, row_count, width_part = states_in.shape
    width = pre_gain.shape[1]
    q_width = w_query.shape[2]
    kv_width = w_key.shape[2]
    sections = lax.axis_size("section")
    tensors = lax.axis_size("tensor")
    seqs = lax.axis_size("seq")
    section_rank = lax.axis_index("section")
    seq_rank = lax.axis_index("seq")
    spans = span_order.shape[0]
    rows = row_count // CHUNKS
    own = rows // tensors
    chunk_len = rows * seqs
    in_steps, out_steps = 4, 4
    in_block, out_block = width // in_steps, width // out_steps
    ids = jnp.arange(spans, dtype=jnp.int32)

    blocks = lax.all_gather(states_in[0], "seq", axis=0).reshape(spans, rows, width_part)
    block_of = jnp.sum(jnp.where(span_order[None, :] == ids[:, None], ids[None, :], 0), axis=1)
    picked = jnp.stack(
        [
            lax.dynamic_index_in_dim(
                blocks,
                lax.dynamic_index_in_dim(block_of, c * seqs + seq_rank, 0, keepdims=False),
                0,
                keepdims=False,
            )
            for c in range(CHUNKS)
        ]
    )
    picked = jnp.moveaxis(picked.reshape(CHUNKS, tensors, own, width_part), 1, 0)
    first_rows = jnp.moveaxis(exchange(picked), 0, 2).reshape(CHUNKS, own, width)

    places = (
        jnp.arange(CHUNKS, dtype=jnp.int32)[:, None] * chunk_len
        + seq_rank * rows
        + jnp.arange(rows, dtype=jnp.int32)[None, :]
    )
    half = HEAD_DIM // 2
    inverse = rotary_base ** (-(jnp.arange(half, dtype=f32) * 2.0 / HEAD_DIM))
    angles = places.astype(f32)[..., None] * inverse
    cos_part, sin_part = jnp.cos(angles), jnp.sin(angles)
    cos_full = jnp.concatenate([cos_part, cos_part], axis=-1)
    sin_full = jnp.concatenate([-sin_part, sin_part], axis=-1)

    key_value = pl.pallas_call(
        key_value_kernel,
        out_shape=(
            jax.ShapeDtypeStruct((rows, 2 * kv_width), bf16),
            jax.ShapeDtypeStruct((rows, width), bf16),
        ),
        in_specs=[SMEM, VMEM, VMEM, VMEM, VMEM, HBM, HBM],
        out_specs=(VMEM, VMEM),
        scratch_shapes=[
            pltpu.VMEM((in_steps, in_block, kv_width), bf16),
            pltpu.VMEM((in_steps, in_block, kv_width), bf16),
            pltpu.SemaphoreType.DMA((2, in_steps)),
        ],
        name="key_value",
    )
    query = pl.pallas_call(
        query_kernel,
        out_shape=jax.ShapeDtypeStruct((rows, q_width), bf16),
        in_specs=[SMEM, VMEM, VMEM, VMEM, HBM],
        out_specs=VMEM,
        scratch_shapes=[
            pltpu.VMEM((in_steps, in_block, q_width), bf16),
            pltpu.SemaphoreType.DMA((in_steps,)),
        ],
        name="query",
    )
    attention = pl.pallas_call(
        attention_kernel,
        out_shape=jax.ShapeDtypeStruct((tensors, own, width), bf16),
        in_specs=[SMEM, VMEM, VMEM, VMEM, VMEM, VMEM, HBM],
        out_specs=VMEM,
        scratch_shapes=[
            pltpu.VMEM((rows, q_width), bf16),
            pltpu.VMEM((out_steps, q_width, out_block), bf16),
            pltpu.SemaphoreType.DMA((out_steps,)),
        ],
        name="attention",
    )
    combine = pl.pallas_call(
        combine_kernel,
        out_shape=jax.ShapeDtypeStruct((own, width), bf16),
        in_specs=[VMEM, VMEM, VMEM],
        out_specs=VMEM,
        name="combine",
    )

    def work(held, past_own, past_other, tick_index):
        slot = jnp.clip(tick_index - section_rank, 0, CHUNKS - 1)
        place = jnp.stack([slot, seq_rank]).astype(jnp.int32)
        full = exchange(jnp.broadcast_to(held[None], (tensors, own, width)))
        kv_own, normed = key_value(place, full, pre_gain, cos_full, sin_full, w_key, w_value)
        kv_other = lax.ppermute(kv_own, "seq", [(0, 1), (1, 0)])
        queries = query(place, normed, cos_full, sin_full, w_query)
        terms = attention(place, queries, kv_own, kv_other, past_own, past_other, w_out)
        return combine(exchange(terms), held, post_gain), kv_own, kv_other

    def tick(carried, tick_index):
        held, past_own, past_other = carried
        new_rows, past_own, past_other = work(held, past_own, past_other, tick_index)
        moved = lax.ppermute(new_rows, "section", [(i, i + 1) for i in range(sections - 1)])
        following = lax.dynamic_index_in_dim(
            first_rows, jnp.minimum(tick_index + 1, CHUNKS - 1), 0, keepdims=False
        )
        held = jnp.where(section_rank == 0, following, moved)
        return (held, past_own, past_other), new_rows

    tick_total = sections + CHUNKS - 1
    no_past = jnp.zeros((rows, 2 * kv_width), bf16)
    carried, made = lax.scan(
        tick, (first_rows[0], no_past, no_past), jnp.arange(tick_total - 1, dtype=jnp.int32)
    )
    last_rows = work(*carried, jnp.int32(tick_total - 1))[0]
    made = jnp.concatenate([made, last_rows[None]], axis=0)
    record = lax.dynamic_slice_in_dim(made, section_rank, CHUNKS, 0)

    pieces = jnp.moveaxis(record.reshape(CHUNKS, own, tensors, width_part), 2, 0)
    pieces = jnp.moveaxis(exchange(pieces), 0, 1).reshape(CHUNKS, rows, width_part)
    ordered = lax.all_gather(pieces, "seq", axis=1).reshape(spans, rows, width_part)
    mine = lax.dynamic_slice_in_dim(span_order, seq_rank * CHUNKS, CHUNKS, 0)
    out = [lax.dynamic_index_in_dim(ordered, mine[j], 0, keepdims=False) for j in range(CHUNKS)]
    return jnp.concatenate(out, axis=0)[None, None]


def solution(mesh):
    in_specs = (
        P(None, "seq", "tensor"),
        P(),
        P("section", None),
        P("section", None, "tensor"),
        P("section", None, "tensor"),
        P("section", None, "tensor"),
        P("section", "tensor", None),
        P("section", None),
    )
    out_specs = P("section", None, "seq", "tensor")
    return jax.shard_map(body, mesh=mesh, in_specs=in_specs, out_specs=out_specs, check_vma=False)
```

```python
import jax
import jax.numpy as jnp
from jax import lax
from jax.experimental import pallas as pl
from jax.experimental.pallas import tpu as pltpu
from jax.sharding import PartitionSpec as P

HEAD_DIM = 128
CHUNKS = 2

softcap_limit = 50.0
query_scale = 144.0 ** (-0.5)
epsilon = 1e-06
rotary_base = 10000.0
f32 = jnp.float32
bf16 = jnp.bfloat16

VMEM = pl.BlockSpec(memory_space=pltpu.VMEM)
SMEM = pl.BlockSpec(memory_space=pltpu.SMEM)
MIB = 1024 * 1024


def limit(mib):
    return pltpu.CompilerParams(vmem_limit_bytes=mib * MIB)


def exchange(pieces, axes):
    return lax.all_to_all(pieces, axes, split_axis=0, concat_axis=0, tiled=True)


def rope(u, cos_full, sin_full):
    return u * cos_full + pltpu.roll(u, HEAD_DIM // 2, 1) * sin_full


def key_value_kernel(place_ref, x_ref, gain_ref, cos_ref, sin_ref, wk_ref, wv_ref,
                     kv_ref, normed_ref):
    rows, width = normed_ref.shape
    kv_width = wk_ref.shape[2]
    x = x_ref[...].astype(f32).reshape(rows, width)
    scaling = lax.rsqrt(jnp.sum(x * x, axis=1, keepdims=True) / width + epsilon)
    normed_ref[...] = (x * scaling * gain_ref[...].astype(f32)).astype(bf16)
    slot = place_ref[0]
    cos_full, sin_full = cos_ref[slot], sin_ref[slot]
    keys = jnp.dot(normed_ref[...], wk_ref[0], preferred_element_type=f32)
    for head in range(kv_width // HEAD_DIM):
        at = slice(head * HEAD_DIM, (head + 1) * HEAD_DIM)
        kv_ref[:, at] = rope(keys[:, at], cos_full, sin_full).astype(bf16)
    values = jnp.dot(normed_ref[...], wv_ref[0], preferred_element_type=f32)
    kv_ref[:, kv_width:] = values.astype(bf16)


def query_kernel(place_ref, normed_ref, cos_ref, sin_ref, wq_ref, q_ref):
    q_width = q_ref.shape[1]
    slot = place_ref[0]
    cos_full, sin_full = cos_ref[slot], sin_ref[slot]
    queries = jnp.dot(normed_ref[...], wq_ref[0], preferred_element_type=f32)
    for head in range(q_width // HEAD_DIM):
        at = slice(head * HEAD_DIM, (head + 1) * HEAD_DIM)
        q_ref[:, at] = (rope(queries[:, at], cos_full, sin_full) * query_scale).astype(bf16)


def attention_kernel(place_ref, q_ref, own_ref, other_ref, past_own_ref, past_other_ref, wo_ref,
                     out_ref, attended_ref):
    rows, q_width = q_ref.shape
    kv_width = own_ref.shape[1] // 2
    kv_heads = kv_width // HEAD_DIM
    group = q_width // kv_width
    has_past = place_ref[0] > 0
    is_later = place_ref[1] > 0
    sources = (own_ref, other_ref, past_own_ref, past_other_ref)
    keys_seen = len(sources) * rows
    row = lax.broadcasted_iota(jnp.int32, (group * rows, keys_seen), 0) % rows
    col = lax.broadcasted_iota(jnp.int32, (group * rows, keys_seen), 1)
    other_to = jnp.where(is_later, 2 * rows, rows)
    past_to = jnp.where(has_past, keys_seen, 2 * rows)
    allowed = (
        ((col < rows) & (col <= row))
        | ((col >= rows) & (col < other_to))
        | ((col >= 2 * rows) & (col < past_to))
    )
    for head in range(kv_heads):
        at = slice(head * HEAD_DIM, (head + 1) * HEAD_DIM)
        value_at = slice(kv_width + head * HEAD_DIM, kv_width + (head + 1) * HEAD_DIM)
        keys = jnp.concatenate([s[:, at] for s in sources], axis=0)
        values = jnp.concatenate([s[:, value_at] for s in sources], axis=0)
        first = head * group * HEAD_DIM
        queries = jnp.concatenate(
            [q_ref[:, first + g * HEAD_DIM:first + (g + 1) * HEAD_DIM] for g in range(group)], axis=0
        )
        scores = lax.dot_general(
            queries, keys, (((1,), (1,)), ((), ())), preferred_element_type=f32
        )
        capped = softcap_limit * jnp.tanh(scores / softcap_limit)
        weight = jnp.where(allowed, jnp.exp(capped), f32(0.0))
        totals = jnp.sum(weight, axis=1, keepdims=True)
        numerator = jnp.dot(weight.astype(bf16), values, preferred_element_type=f32)
        attended = (numerator / totals).astype(bf16)
        for g in range(group):
            attended_ref[:, first + g * HEAD_DIM:first + (g + 1) * HEAD_DIM] = attended[
                g * rows:(g + 1) * rows
            ]
    terms = jnp.dot(attended_ref[...], wo_ref[0], preferred_element_type=f32)
    out_ref[...] = terms.reshape(out_ref.shape).astype(bf16)


def combine_kernel(arrived_ref, held_ref, gain_ref, out_ref):
    width = out_ref.shape[1]
    projected = jnp.sum(arrived_ref[...].astype(f32), axis=0)
    mean = jnp.sum(projected * projected, axis=1, keepdims=True) / width
    scaled = projected * lax.rsqrt(mean + epsilon) * gain_ref[...].astype(f32)
    out_ref[...] = (held_ref[...].astype(f32) + scaled).astype(bf16)


def pick_kernel(order_ref, place_ref, blocks_ref, out_ref):
    peers, _, _ = out_ref.shape
    spans, rows, _ = blocks_ref.shape
    own = rows // peers
    core = place_ref[1]
    block_of = []
    for chunk in range(CHUNKS):
        span = core + chunk * (spans // CHUNKS)
        at = jnp.int32(0)
        for j in range(1, spans):
            at = jnp.where(order_ref[j] == span, j, at)
        block_of.append(at)
    first = blocks_ref[block_of[0]]
    second = blocks_ref[block_of[1]].astype(f32)
    for t in range(peers):
        out_ref[t, :rows] = first
        out_ref[t, rows:] = second[t * own:(t + 1) * own].astype(bf16)


def gather_kernel(place_ref, arrived_ref, full_ref, held_ref, next_ref):
    peers, own, width = full_ref.shape
    rows = peers * own
    part = width // peers
    for t in range(peers):
        at = slice(t * part, (t + 1) * part)
        piece = arrived_ref[t].astype(f32)
        full_ref[:, :, at] = piece[:rows].reshape(peers, own, part).astype(bf16)
        next_ref[:, at] = piece[rows:].astype(bf16)
    held_ref[...] = full_ref[place_ref[2]]


def split_kernel(place_ref, *refs):
    *made_refs, out_ref = refs
    cores, peers, chunks, own, part = out_ref.shape
    section = place_ref[3]
    for chunk in range(chunks):
        rows = made_refs[chunk][...].astype(f32)
        for i in range(1, len(made_refs) - chunks + 1):
            rows = jnp.where(section == i, made_refs[i + chunk][...].astype(f32), rows)
        for t in range(peers):
            piece = rows[:, t * part:(t + 1) * part].astype(bf16)
            for core in range(cores):
                out_ref[core, t, chunk] = piece


def order_kernel(order_ref, place_ref, arrived_ref, out_ref):
    cores, peers, chunks, own, part = arrived_ref.shape
    rows = peers * own
    blocks = out_ref.shape[0] // rows
    for j in range(blocks):
        span = order_ref[place_ref[1] * blocks + j]
        chunk, core = lax.div(span, jnp.int32(cores)), lax.rem(span, jnp.int32(cores))
        piece = arrived_ref[core, :, chunk].astype(f32).reshape(rows, part)
        out_ref[j * rows:(j + 1) * rows] = piece.astype(bf16)


def body(states_in, span_order, pre_gain, w_query, w_key, w_value, w_out, post_gain):
    _, row_count, part = states_in.shape
    width = pre_gain.shape[1]
    q_width = w_query.shape[2]
    kv_width = w_key.shape[2]
    sections = lax.axis_size("section")
    tensors = lax.axis_size("tensor")
    seqs = lax.axis_size("seq")
    section_rank = lax.axis_index("section")
    seq_rank = lax.axis_index("seq")
    tensor_rank = lax.axis_index("tensor")
    spans = span_order.shape[0]
    rows = row_count // CHUNKS
    own = rows // tensors
    chunk_len = rows * seqs

    key_value = pl.pallas_call(
        key_value_kernel,
        out_shape=(
            jax.ShapeDtypeStruct((rows, 2 * kv_width), bf16),
            jax.ShapeDtypeStruct((rows, width), bf16),
        ),
        in_specs=[SMEM] + [VMEM] * 6,
        out_specs=(VMEM, VMEM),
        compiler_params=limit(10),
        name="key_value",
    )
    query = pl.pallas_call(
        query_kernel,
        out_shape=jax.ShapeDtypeStruct((rows, q_width), bf16),
        in_specs=[SMEM] + [VMEM] * 4,
        out_specs=VMEM,
        compiler_params=limit(8),
        name="query",
    )
    attention = pl.pallas_call(
        attention_kernel,
        out_shape=jax.ShapeDtypeStruct((tensors, own, width), bf16),
        in_specs=[SMEM] + [VMEM] * 6,
        out_specs=VMEM,
        scratch_shapes=[pltpu.VMEM((rows, q_width), bf16)],
        compiler_params=limit(10),
        name="attention",
    )
    combine = pl.pallas_call(
        combine_kernel,
        out_shape=jax.ShapeDtypeStruct((own, width), bf16),
        in_specs=[VMEM, VMEM, VMEM],
        out_specs=VMEM,
        compiler_params=limit(4),
        name="combine",
    )

    tick_total = sections + CHUNKS - 1
    slots = jnp.clip(jnp.arange(tick_total, dtype=jnp.int32) - section_rank, 0, CHUNKS - 1)
    ranks = jnp.stack([seq_rank, tensor_rank, section_rank]).astype(jnp.int32)
    place_all = jnp.concatenate(
        [slots[:, None], jnp.broadcast_to(ranks[None], (tick_total, 3))], axis=1
    )
    places = (
        jnp.arange(CHUNKS, dtype=jnp.int32)[:, None] * chunk_len
        + seq_rank * rows
        + jnp.arange(rows, dtype=jnp.int32)[None, :]
    )
    half = HEAD_DIM // 2
    inverse = rotary_base ** (-(jnp.arange(half, dtype=f32) * 2.0 / HEAD_DIM))
    angles = places.astype(f32)[..., None] * inverse
    cos_part, sin_part = jnp.cos(angles), jnp.sin(angles)
    cos_full = jnp.concatenate([cos_part, cos_part], axis=-1)
    sin_full = jnp.concatenate([-sin_part, sin_part], axis=-1)

    blocks = lax.all_gather(states_in[0], "seq", axis=0).reshape(spans, rows, part)
    pieces = pl.pallas_call(
        pick_kernel,
        out_shape=jax.ShapeDtypeStruct((tensors, rows + own, part), bf16),
        in_specs=[SMEM, SMEM, VMEM],
        out_specs=VMEM,
        compiler_params=limit(4),
        name="pick",
    )(span_order, place_all[0], blocks)
    pieces, place_all, cos_full, sin_full = lax.optimization_barrier(
        (pieces, place_all, cos_full, sin_full)
    )
    full, held, following = pl.pallas_call(
        gather_kernel,
        out_shape=(
            jax.ShapeDtypeStruct((tensors, own, width), bf16),
            jax.ShapeDtypeStruct((own, width), bf16),
            jax.ShapeDtypeStruct((own, width), bf16),
        ),
        in_specs=[SMEM, VMEM],
        out_specs=(VMEM, VMEM, VMEM),
        compiler_params=limit(6),
        name="gather",
    )(place_all[0], exchange(pieces, "tensor"))

    past = (jnp.zeros((rows, 2 * kv_width), bf16),) * 2
    made = []
    for tick in range(tick_total):
        place = place_all[tick]
        kv_own, normed = key_value(place, full, pre_gain, cos_full, sin_full, w_key, w_value)
        kv_other = lax.ppermute(kv_own, "seq", [(0, 1), (1, 0)])
        queries = query(place, normed, cos_full, sin_full, w_query)
        terms = attention(place, queries, kv_own, kv_other, *past, w_out)
        past = (kv_own, kv_other)
        made.append(combine(exchange(terms, "tensor"), held, post_gain))
        if tick + 1 < tick_total:
            busy = [i for i in range(sections - 1) if 0 <= tick - i < CHUNKS]
            held = lax.ppermute(made[-1], "section", [(i, i + 1) for i in busy])
            if tick + 1 < CHUNKS:
                held = jnp.where(section_rank == 0, following, held)
            full = exchange(jnp.broadcast_to(held[None], (tensors, own, width)), "tensor")

    made = lax.optimization_barrier(tuple(made))
    pieces = pl.pallas_call(
        split_kernel,
        out_shape=jax.ShapeDtypeStruct((seqs, tensors, CHUNKS, own, part), bf16),
        in_specs=[SMEM] + [VMEM] * tick_total,
        out_specs=VMEM,
        compiler_params=limit(6),
        name="split",
    )(place_all[0], *made)
    pieces = exchange(pieces.reshape(seqs * tensors, CHUNKS, own, part), ("seq", "tensor"))
    out = pl.pallas_call(
        order_kernel,
        out_shape=jax.ShapeDtypeStruct((row_count, part), bf16),
        in_specs=[SMEM, SMEM, VMEM],
        out_specs=VMEM,
        compiler_params=limit(4),
        name="order",
    )(span_order, place_all[0], pieces.reshape(seqs, tensors, CHUNKS, own, part))
    return out[None, None]


def solution(mesh):
    in_specs = (
        P(None, "seq", "tensor"),
        P(),
        P("section", None),
        P("section", None, "tensor"),
        P("section", None, "tensor"),
        P("section", None, "tensor"),
        P("section", "tensor", None),
        P("section", None),
    )
    out_specs = P("section", None, "seq", "tensor")
    return jax.shard_map(body, mesh=mesh, in_specs=in_specs, out_specs=out_specs, check_vma=False)
```

```python
import functools

import jax
import jax.numpy as jnp
from jax import lax
from jax.experimental import pallas as pl
from jax.experimental.pallas import tpu as pltpu
from jax.sharding import PartitionSpec as P

HEAD_DIM = 128
CHUNKS = 2
LANES = 128
OWN = 8

softcap_limit = 50.0
query_scale = 144.0 ** (-0.5)
epsilon = 1e-06
rotary_base = 10000.0
f32 = jnp.float32
bf16 = jnp.bfloat16

VMEM = pl.BlockSpec(memory_space=pltpu.VMEM)

FIRST_FROM, SECOND_FROM, GIVEN_AS = 0, 4, 8
SECTION, CORE, OWNER, FACTS = 16, 17, 18, 24
MIB = 1024 * 1024


def limit(mib):
    return pltpu.CompilerParams(vmem_limit_bytes=mib * MIB)


def exchange(pieces, axes):
    return lax.all_to_all(pieces, axes, split_axis=0, concat_axis=0, tiled=True)


def tiles(ref_shape):
    return range(ref_shape[-2] // OWN)


def tile(c):
    return slice(c * OWN, (c + 1) * OWN)


def fact(facts_ref, row):
    return facts_ref[row:row + 1, :]


def one_of(facts_ref, first, choices):
    picked = choices[0]
    for i in range(1, len(choices)):
        picked = jnp.where(facts_ref[first + i:first + i + 1, :1] > 0, choices[i], picked)
    return picked


def is_later(facts_ref, tick):
    return fact(facts_ref, SECTION) <= tick - 1


def lanes(c):
    return slice(c * LANES, (c + 1) * LANES)


def rope(u, cos_full, sin_full):
    return u * cos_full + pltpu.roll(u, HEAD_DIM // 2, 1) * sin_full


def key_value_kernel(tick, facts_ref, x_ref, gain_ref, cos_ref, sin_ref, wk_ref, wv_ref,
                     kv_ref, normed_ref):
    rows, width = normed_ref.shape
    kv_width = wk_ref.shape[2]
    squares = jnp.zeros((rows, LANES), f32)
    for c in tiles(x_ref.shape):
        x = x_ref[:, tile(c)].astype(f32).reshape(rows, LANES)
        squares += x * x
    scaling = lax.rsqrt(jnp.sum(squares, axis=1, keepdims=True) / width + epsilon)
    for c in tiles(x_ref.shape):
        x = x_ref[:, tile(c)].astype(f32).reshape(rows, LANES)
        normed_ref[:, lanes(c)] = (x * scaling * gain_ref[:, lanes(c)].astype(f32)).astype(bf16)
    later = is_later(facts_ref, tick)
    cos_full = jnp.where(later, cos_ref[1], cos_ref[0])
    sin_full = jnp.where(later, sin_ref[1], sin_ref[0])
    keys = jnp.dot(normed_ref[...], wk_ref[0], preferred_element_type=f32)
    for head in range(kv_width // HEAD_DIM):
        at = slice(head * HEAD_DIM, (head + 1) * HEAD_DIM)
        kv_ref[:, at] = rope(keys[:, at], cos_full, sin_full).astype(bf16)
    values = jnp.dot(normed_ref[...], wv_ref[0], preferred_element_type=f32)
    kv_ref[:, kv_width:] = values.astype(bf16)


def query_kernel(tick, facts_ref, normed_ref, cos_ref, sin_ref, wq_ref, q_ref):
    q_width = q_ref.shape[1]
    later = is_later(facts_ref, tick)
    cos_full = jnp.where(later, cos_ref[1], cos_ref[0])
    sin_full = jnp.where(later, sin_ref[1], sin_ref[0])
    queries = jnp.dot(normed_ref[...], wq_ref[0], preferred_element_type=f32)
    for head in range(q_width // HEAD_DIM):
        at = slice(head * HEAD_DIM, (head + 1) * HEAD_DIM)
        q_ref[:, at] = (rope(queries[:, at], cos_full, sin_full) * query_scale).astype(bf16)


def attention_kernel(tick, facts_ref, q_ref, own_ref, other_ref, past_own_ref, past_other_ref, wo_ref,
                     out_ref, attended_ref):
    rows, q_width = q_ref.shape
    kv_width = own_ref.shape[1] // 2
    kv_heads = kv_width // HEAD_DIM
    group = q_width // kv_width
    sources = (own_ref, other_ref, past_own_ref, past_other_ref)
    half = 2 * rows
    row = lax.broadcasted_iota(jnp.int32, (group * rows, half), 0) % rows
    col = lax.broadcasted_iota(jnp.int32, (group * rows, half), 1)
    after = jnp.broadcast_to(fact(facts_ref, CORE) > 0, (group * rows, half))
    has_past = jnp.broadcast_to(is_later(facts_ref, tick), (group * rows, half))
    now = ((col < rows) & (col <= row)) | ((col >= rows) & after)
    for head in range(kv_heads):
        at = slice(head * HEAD_DIM, (head + 1) * HEAD_DIM)
        value_at = slice(kv_width + head * HEAD_DIM, kv_width + (head + 1) * HEAD_DIM)
        keys = jnp.concatenate([s[:, at] for s in sources], axis=0)
        values = jnp.concatenate([s[:, value_at] for s in sources], axis=0)
        first = head * group * HEAD_DIM
        queries = jnp.concatenate(
            [q_ref[:, first + g * HEAD_DIM:first + (g + 1) * HEAD_DIM] for g in range(group)], axis=0
        )
        scores = lax.dot_general(
            queries, keys, (((1,), (1,)), ((), ())), preferred_element_type=f32
        )
        capped = softcap_limit * jnp.tanh(scores / softcap_limit)
        weight = jnp.exp(capped)
        weight = jnp.concatenate(
            [
                jnp.where(now, weight[:, :half], f32(0.0)),
                jnp.where(has_past, weight[:, half:], f32(0.0)),
            ],
            axis=1,
        )
        totals = jnp.sum(weight, axis=1, keepdims=True)
        numerator = jnp.dot(weight.astype(bf16), values, preferred_element_type=f32)
        attended = (numerator / totals).astype(bf16)
        for g in range(group):
            attended_ref[:, first + g * HEAD_DIM:first + (g + 1) * HEAD_DIM] = attended[
                g * rows:(g + 1) * rows
            ]
    terms = jnp.dot(attended_ref[...], wo_ref[0], preferred_element_type=f32)
    for c in tiles(out_ref.shape):
        out_ref[:, tile(c)] = terms[:, lanes(c)].reshape(-1, OWN, LANES).astype(bf16)


def combine_kernel(arrived_ref, held_ref, gain_ref, out_ref, sum_ref):
    width = gain_ref.shape[1]
    squares = jnp.zeros((OWN, LANES), f32)
    for c in tiles(out_ref.shape):
        projected = jnp.sum(arrived_ref[:, tile(c)].astype(f32), axis=0)
        sum_ref[tile(c)] = projected
        squares += projected * projected
    scaling = lax.rsqrt(jnp.sum(squares, axis=1, keepdims=True) / width + epsilon)
    for c in tiles(out_ref.shape):
        scaled = sum_ref[tile(c)] * scaling * gain_ref[:, lanes(c)].astype(f32)
        out_ref[tile(c)] = (held_ref[tile(c)].astype(f32) + scaled).astype(bf16)


def choose_kernel(facts_ref, moved_ref, following_ref, held_ref):
    is_first = fact(facts_ref, SECTION) < 1
    moved, following = moved_ref[...].astype(f32), following_ref[...].astype(f32)
    held_ref[...] = jnp.where(is_first, following, moved).astype(bf16)


def pick_kernel(facts_ref, blocks_ref, out_ref):
    peers = out_ref.shape[0]
    spans, rows, _ = blocks_ref.shape
    blocks = [blocks_ref[j].astype(f32) for j in range(spans)]
    first = one_of(facts_ref, FIRST_FROM, blocks).astype(bf16)
    second = one_of(facts_ref, SECOND_FROM, blocks)
    for t in range(peers):
        out_ref[t, :rows] = first
        out_ref[t, rows:] = second[t * OWN:(t + 1) * OWN].astype(bf16)


def gather_kernel(facts_ref, arrived_ref, full_ref, held_ref, next_ref, flat_ref):
    peers = full_ref.shape[0]
    rows = peers * OWN
    part = flat_ref.shape[1] // peers
    for t in range(peers):
        flat_ref[:, t * part:(t + 1) * part] = arrived_ref[t].astype(f32)
    owner = fact(facts_ref, OWNER)
    for c in tiles(next_ref.shape):
        blocks = flat_ref[:rows, lanes(c)].reshape(peers, OWN, LANES)
        full_ref[:, tile(c)] = blocks.astype(bf16)
        held = blocks[0]
        for t in range(1, peers):
            held = jnp.where(owner == t, blocks[t], held)
        held_ref[tile(c)] = held.astype(bf16)
        next_ref[tile(c)] = flat_ref[rows:, lanes(c)].astype(bf16)


def split_kernel(facts_ref, *refs):
    *made_refs, out_ref, flat_ref = refs
    cores, peers, chunks, _, part = out_ref.shape
    section = fact(facts_ref, SECTION)
    for chunk in range(chunks):
        rows = made_refs[chunk][...].astype(f32)
        for i in range(1, len(made_refs) - chunks + 1):
            rows = jnp.where(section == i, made_refs[i + chunk][...].astype(f32), rows)
        for c in tiles(rows.shape):
            flat_ref[:, lanes(c)] = rows[tile(c)]
        for t in range(peers):
            piece = flat_ref[:, t * part:(t + 1) * part].astype(bf16)
            for core in range(cores):
                out_ref[core, t, chunk] = piece


def order_kernel(facts_ref, arrived_ref, out_ref):
    cores, peers, chunks, _, part = arrived_ref.shape
    rows = peers * OWN
    spans = [
        arrived_ref[core, :, chunk].astype(f32).reshape(rows, part)
        for chunk in range(chunks)
        for core in range(cores)
    ]
    for j in range(out_ref.shape[0] // rows):
        piece = one_of(facts_ref, GIVEN_AS + j * len(spans), spans)
        out_ref[j * rows:(j + 1) * rows] = piece.astype(bf16)


def body(states_in, span_order, pre_gain, w_query, w_key, w_value, w_out, post_gain):
    _, row_count, part = states_in.shape
    width = pre_gain.shape[1]
    q_width = w_query.shape[2]
    kv_width = w_key.shape[2]
    sections = lax.axis_size("section")
    tensors = lax.axis_size("tensor")
    seqs = lax.axis_size("seq")
    section_rank = lax.axis_index("section")
    seq_rank = lax.axis_index("seq")
    tensor_rank = lax.axis_index("tensor")
    spans = span_order.shape[0]
    rows = row_count // CHUNKS
    own = rows // tensors
    assert own == OWN
    chunk_len = rows * seqs
    block = (own * width // LANES, LANES)

    key_value = lambda tick: pl.pallas_call(
        functools.partial(key_value_kernel, tick),
        out_shape=(
            jax.ShapeDtypeStruct((rows, 2 * kv_width), bf16),
            jax.ShapeDtypeStruct((rows, width), bf16),
        ),
        in_specs=[VMEM] * 7,
        out_specs=(VMEM, VMEM),
        compiler_params=limit(10),
        name="key_value",
    )
    query = lambda tick: pl.pallas_call(
        functools.partial(query_kernel, tick),
        out_shape=jax.ShapeDtypeStruct((rows, q_width), bf16),
        in_specs=[VMEM] * 5,
        out_specs=VMEM,
        compiler_params=limit(8),
        name="query",
    )
    attention = lambda tick: pl.pallas_call(
        functools.partial(attention_kernel, tick),
        out_shape=jax.ShapeDtypeStruct((tensors, *block), bf16),
        in_specs=[VMEM] * 7,
        out_specs=VMEM,
        scratch_shapes=[pltpu.VMEM((rows, q_width), bf16)],
        compiler_params=limit(10),
        name="attention",
    )
    combine = pl.pallas_call(
        combine_kernel,
        out_shape=jax.ShapeDtypeStruct(block, bf16),
        in_specs=[VMEM, VMEM, VMEM],
        out_specs=VMEM,
        scratch_shapes=[pltpu.VMEM(block, f32)],
        compiler_params=limit(4),
        name="combine",
    )

    tick_total = sections + CHUNKS - 1
    ids = jnp.arange(spans, dtype=jnp.int32)
    given = lax.dynamic_slice_in_dim(span_order, seq_rank * (spans // seqs), spans // seqs, 0)
    rows_of_facts = [span_order == chunk * seqs + seq_rank for chunk in range(CHUNKS)]
    rows_of_facts += [(given[:, None] == ids[None, :]).reshape(-1)]
    rows_of_facts += [jnp.stack([section_rank, seq_rank, tensor_rank])]
    facts = jnp.concatenate([r.astype(f32) for r in rows_of_facts])
    facts = jnp.pad(facts, (0, FACTS - facts.shape[0]))
    facts = jnp.broadcast_to(facts[:, None], (FACTS, LANES))
    places = (
        jnp.arange(CHUNKS, dtype=jnp.int32)[:, None] * chunk_len
        + seq_rank * rows
        + jnp.arange(rows, dtype=jnp.int32)[None, :]
    )
    half = HEAD_DIM // 2
    inverse = rotary_base ** (-(jnp.arange(half, dtype=f32) * 2.0 / HEAD_DIM))
    angles = places.astype(f32)[..., None] * inverse
    cos_part, sin_part = jnp.cos(angles), jnp.sin(angles)
    cos_full = jnp.concatenate([cos_part, cos_part], axis=-1)
    sin_full = jnp.concatenate([-sin_part, sin_part], axis=-1)

    blocks = lax.all_gather(states_in[0], "seq", axis=0).reshape(spans, rows, part)
    pieces = pl.pallas_call(
        pick_kernel,
        out_shape=jax.ShapeDtypeStruct((tensors, rows + own, part), bf16),
        in_specs=[VMEM, VMEM],
        out_specs=VMEM,
        compiler_params=limit(4),
        name="pick",
    )(facts, blocks)
    no_past = jnp.zeros((rows, 2 * kv_width), bf16)
    pieces, facts, cos_full, sin_full, no_past = lax.optimization_barrier(
        (pieces, facts, cos_full, sin_full, no_past)
    )
    full, held, following = pl.pallas_call(
        gather_kernel,
        out_shape=(
            jax.ShapeDtypeStruct((tensors, *block), bf16),
            jax.ShapeDtypeStruct(block, bf16),
            jax.ShapeDtypeStruct(block, bf16),
        ),
        in_specs=[VMEM, VMEM],
        out_specs=(VMEM, VMEM, VMEM),
        scratch_shapes=[pltpu.VMEM((rows + own, width), f32)],
        compiler_params=limit(6),
        name="gather",
    )(facts, exchange(pieces, "tensor"))

    past = (no_past, no_past)
    made = []
    for tick in range(tick_total):
        kv_own, normed = key_value(tick)(facts, full, pre_gain, cos_full, sin_full, w_key, w_value)
        kv_other = lax.ppermute(kv_own, "seq", [(0, 1), (1, 0)])
        queries = query(tick)(facts, normed, cos_full, sin_full, w_query)
        terms = attention(tick)(facts, queries, kv_own, kv_other, *past, w_out)
        past = (kv_own, kv_other)
        made.append(combine(exchange(terms, "tensor"), held, post_gain))
        if tick + 1 < tick_total:
            busy = [i for i in range(sections - 1) if 0 <= tick - i < CHUNKS]
            held = lax.ppermute(made[-1], "section", [(i, i + 1) for i in busy])
            if tick + 1 < CHUNKS:
                held = pl.pallas_call(
                    choose_kernel,
                    out_shape=jax.ShapeDtypeStruct(block, bf16),
                    in_specs=[VMEM] * 3,
                    out_specs=VMEM,
                    compiler_params=limit(2),
                    name="choose",
                )(facts, held, following)
            full = exchange(jnp.broadcast_to(held[None], (tensors, *block)), "tensor")

    made = lax.optimization_barrier(tuple(made))
    pieces = pl.pallas_call(
        split_kernel,
        out_shape=jax.ShapeDtypeStruct((seqs, tensors, CHUNKS, own, part), bf16),
        in_specs=[VMEM] * (tick_total + 1),
        out_specs=VMEM,
        scratch_shapes=[pltpu.VMEM((own, width), f32)],
        compiler_params=limit(6),
        name="split",
    )(facts, *made)
    pieces = exchange(pieces.reshape(seqs * tensors, CHUNKS, own, part), ("seq", "tensor"))
    out = pl.pallas_call(
        order_kernel,
        out_shape=jax.ShapeDtypeStruct((row_count, part), bf16),
        in_specs=[VMEM, VMEM],
        out_specs=VMEM,
        compiler_params=limit(4),
        name="order",
    )(facts, pieces.reshape(seqs, tensors, CHUNKS, own, part))
    return out[None, None]


def solution(mesh):
    in_specs = (
        P(None, "seq", "tensor"),
        P(),
        P("section", None),
        P("section", None, "tensor"),
        P("section", None, "tensor"),
        P("section", None, "tensor"),
        P("section", "tensor", None),
        P("section", None),
    )
    out_specs = P("section", None, "seq", "tensor")
    return jax.shard_map(body, mesh=mesh, in_specs=in_specs, out_specs=out_specs, check_vma=False)
```

```python
import functools

import jax
import jax.numpy as jnp
from jax import lax
from jax.experimental import pallas as pl
from jax.experimental.pallas import tpu as pltpu
from jax.sharding import PartitionSpec as P

HEAD_DIM = 128
CHUNKS = 2
LANES = 128
OWN = 8
FOLD = 5

softcap_limit = 50.0
query_scale = 144.0 ** (-0.5)
epsilon = 1e-06
rotary_base = 10000.0
f32 = jnp.float32
bf16 = jnp.bfloat16

VMEM = pl.BlockSpec(memory_space=pltpu.VMEM)

FIRST_FROM, SECOND_FROM, GIVEN_AS = 0, 4, 8
SECTION, CORE, OWNER, FACTS = 16, 17, 18, 24
MIB = 1024 * 1024


def limit(mib):
    return pltpu.CompilerParams(vmem_limit_bytes=mib * MIB)


def exchange(pieces, axes):
    return lax.all_to_all(pieces, axes, split_axis=0, concat_axis=0, tiled=True)


def tiles(ref_shape):
    return range(ref_shape[-2] // OWN)


def tile(c):
    return slice(c * OWN, (c + 1) * OWN)


def fact(facts_ref, row):
    return facts_ref[row:row + 1, :]


def one_of(facts_ref, first, choices):
    picked = choices[0]
    for i in range(1, len(choices)):
        picked = jnp.where(facts_ref[first + i:first + i + 1, :1] > 0, choices[i], picked)
    return picked


def is_later(facts_ref, tick):
    return fact(facts_ref, SECTION) <= tick - 1


def lanes(c):
    return slice(c * LANES, (c + 1) * LANES)


def rope(u, cos_full, sin_full):
    return u * cos_full + pltpu.roll(u, HEAD_DIM // 2, 1) * sin_full


def key_value_kernel(tick, facts_ref, x_ref, gain_ref, cos_ref, sin_ref, wk_ref, wv_ref,
                     kv_ref, normed_ref):
    rows, width = normed_ref.shape
    kv_width = wk_ref.shape[2]
    squares = jnp.zeros((rows, LANES), f32)
    for c in tiles(x_ref.shape):
        x = x_ref[:, tile(c)].astype(f32).reshape(rows, LANES)
        squares += x * x
    scaling = lax.rsqrt(jnp.sum(squares, axis=1, keepdims=True) / width + epsilon)
    for c in tiles(x_ref.shape):
        x = x_ref[:, tile(c)].astype(f32).reshape(rows, LANES)
        normed_ref[:, lanes(c)] = (x * scaling * gain_ref[:, lanes(c)].astype(f32)).astype(bf16)
    later = is_later(facts_ref, tick)
    cos_full = jnp.where(later, cos_ref[1], cos_ref[0])
    sin_full = jnp.where(later, sin_ref[1], sin_ref[0])
    keys = jnp.dot(normed_ref[...], wk_ref[0], preferred_element_type=f32)
    for head in range(kv_width // HEAD_DIM):
        at = slice(head * HEAD_DIM, (head + 1) * HEAD_DIM)
        kv_ref[:, at] = rope(keys[:, at], cos_full, sin_full).astype(bf16)
    values = jnp.dot(normed_ref[...], wv_ref[0], preferred_element_type=f32)
    kv_ref[:, kv_width:] = values.astype(bf16)


def query_kernel(tick, facts_ref, normed_ref, cos_ref, sin_ref, wq_ref, q_ref):
    q_width = q_ref.shape[1]
    later = is_later(facts_ref, tick)
    cos_full = jnp.where(later, cos_ref[1], cos_ref[0])
    sin_full = jnp.where(later, sin_ref[1], sin_ref[0])
    queries = jnp.dot(normed_ref[...], wq_ref[0], preferred_element_type=f32)
    for head in range(q_width // HEAD_DIM):
        at = slice(head * HEAD_DIM, (head + 1) * HEAD_DIM)
        q_ref[:, at] = (rope(queries[:, at], cos_full, sin_full) * query_scale).astype(bf16)


def attention_kernel(tick, facts_ref, q_ref, own_ref, other_ref, past_own_ref, past_other_ref, wo_ref,
                     out_ref, attended_ref):
    rows, q_width = q_ref.shape
    kv_width = own_ref.shape[1] // 2
    kv_heads = kv_width // HEAD_DIM
    group = q_width // kv_width
    sources = (own_ref, other_ref, past_own_ref, past_other_ref)
    half = 2 * rows
    row = lax.broadcasted_iota(jnp.int32, (group * rows, half), 0) % rows
    col = lax.broadcasted_iota(jnp.int32, (group * rows, half), 1)
    after = jnp.broadcast_to(fact(facts_ref, CORE) > 0, (group * rows, half))
    has_past = jnp.broadcast_to(is_later(facts_ref, tick), (group * rows, half))
    now = ((col < rows) & (col <= row)) | ((col >= rows) & after)
    for head in range(kv_heads):
        at = slice(head * HEAD_DIM, (head + 1) * HEAD_DIM)
        value_at = slice(kv_width + head * HEAD_DIM, kv_width + (head + 1) * HEAD_DIM)
        keys = jnp.concatenate([s[:, at] for s in sources], axis=0)
        values = jnp.concatenate([s[:, value_at] for s in sources], axis=0)
        first = head * group * HEAD_DIM
        queries = jnp.concatenate(
            [q_ref[:, first + g * HEAD_DIM:first + (g + 1) * HEAD_DIM] for g in range(group)], axis=0
        )
        scores = lax.dot_general(
            queries, keys, (((1,), (1,)), ((), ())), preferred_element_type=f32
        )
        capped = softcap_limit * jnp.tanh(scores / softcap_limit)
        weight = jnp.exp(capped)
        weight = jnp.concatenate(
            [
                jnp.where(now, weight[:, :half], f32(0.0)),
                jnp.where(has_past, weight[:, half:], f32(0.0)),
            ],
            axis=1,
        )
        totals = jnp.sum(weight, axis=1, keepdims=True)
        numerator = jnp.dot(weight.astype(bf16), values, preferred_element_type=f32)
        attended = (numerator / totals).astype(bf16)
        for g in range(group):
            attended_ref[:, first + g * HEAD_DIM:first + (g + 1) * HEAD_DIM] = attended[
                g * rows:(g + 1) * rows
            ]
    terms = jnp.dot(attended_ref[...], wo_ref[0], preferred_element_type=f32)
    for c in tiles(out_ref.shape):
        out_ref[:, tile(c)] = terms[:, lanes(c)].reshape(-1, OWN, LANES).astype(bf16)


def combine_kernel(arrived_ref, held_ref, gain_ref, out_ref, sum_ref):
    width = gain_ref.shape[1]
    squares = jnp.zeros((OWN, LANES), f32)
    for c in tiles(out_ref.shape):
        projected = jnp.sum(arrived_ref[:, tile(c)].astype(f32), axis=0)
        sum_ref[tile(c)] = projected
        squares += projected * projected
    scaling = lax.rsqrt(jnp.sum(squares, axis=1, keepdims=True) / width + epsilon)
    for c in tiles(out_ref.shape):
        scaled = sum_ref[tile(c)] * scaling * gain_ref[:, lanes(c)].astype(f32)
        out_ref[tile(c)] = (held_ref[tile(c)].astype(f32) + scaled).astype(bf16)


def choose_kernel(facts_ref, moved_ref, following_ref, held_ref):
    is_first = fact(facts_ref, SECTION) < 1
    moved, following = moved_ref[...].astype(f32), following_ref[...].astype(f32)
    held_ref[...] = jnp.where(is_first, following, moved).astype(bf16)


def pick_kernel(facts_ref, mine_ref, theirs_ref, out_ref):
    peers = out_ref.shape[0]
    both = [jnp.transpose(ref[...].astype(f32)) for ref in (mine_ref, theirs_ref)]
    rows = both[0].shape[0] // CHUNKS
    part = both[0].shape[1]
    blocks = [b[i * rows:(i + 1) * rows] for b in both for i in range(CHUNKS)]
    first = one_of(facts_ref, FIRST_FROM, blocks)
    second = one_of(facts_ref, SECOND_FROM, blocks)
    sent, whole = rows + OWN, part // LANES
    kept = FOLD * OWN
    for t in range(peers):
        own = second[t * OWN:(t + 1) * OWN]
        for c in range(whole):
            out_ref[t, c * sent:c * sent + rows] = first[:, lanes(c)].astype(bf16)
            out_ref[t, c * sent + rows:(c + 1) * sent] = own[:, lanes(c)].astype(bf16)
        rest = slice(whole * LANES, part)
        upper = jnp.concatenate([first[kept:, rest], own[:, rest], own[:, rest]], axis=0)
        fold = jnp.concatenate([first[:kept, rest], upper], axis=1)
        out_ref[t, whole * sent:] = fold.astype(bf16)


def gather_kernel(facts_ref, arrived_ref, full_ref, held_ref, next_ref, flat_ref):
    peers = full_ref.shape[0]
    rows = peers * OWN
    part = flat_ref.shape[1] // peers
    sent, whole = rows + OWN, part // LANES
    kept = FOLD * OWN
    rest = part - whole * LANES
    for t in range(peers):
        for c in range(whole):
            piece = arrived_ref[t, c * sent:(c + 1) * sent].astype(f32)
            flat_ref[:, t * part + c * LANES:t * part + (c + 1) * LANES] = piece
        fold = arrived_ref[t, whole * sent:].astype(f32)
        at = slice((t + 1) * part - rest, (t + 1) * part)
        flat_ref[:kept, at] = fold[:, :rest]
        flat_ref[kept:, at] = fold[:sent - kept, rest:]
    owner = fact(facts_ref, OWNER)
    for c in tiles(next_ref.shape):
        blocks = flat_ref[:rows, lanes(c)].reshape(peers, OWN, LANES)
        full_ref[:, tile(c)] = blocks.astype(bf16)
        held = blocks[0]
        for t in range(1, peers):
            held = jnp.where(owner == t, blocks[t], held)
        held_ref[tile(c)] = held.astype(bf16)
        next_ref[tile(c)] = flat_ref[rows:, lanes(c)].astype(bf16)


def split_kernel(facts_ref, *refs):
    *made_refs, out_ref, flat_ref = refs
    cores, peers, chunks, _, part = out_ref.shape
    section = fact(facts_ref, SECTION)
    for chunk in range(chunks):
        rows = made_refs[chunk][...].astype(f32)
        for i in range(1, len(made_refs) - chunks + 1):
            rows = jnp.where(section == i, made_refs[i + chunk][...].astype(f32), rows)
        for c in tiles(rows.shape):
            flat_ref[:, lanes(c)] = rows[tile(c)]
        for t in range(peers):
            piece = flat_ref[:, t * part:(t + 1) * part].astype(bf16)
            for core in range(cores):
                out_ref[core, t, chunk] = piece


def order_kernel(facts_ref, arrived_ref, out_ref):
    cores, peers, chunks, _, part = arrived_ref.shape
    rows = peers * OWN
    spans = [
        arrived_ref[core, :, chunk].astype(f32).reshape(rows, part)
        for chunk in range(chunks)
        for core in range(cores)
    ]
    blocks = out_ref.shape[1] // rows
    given = [one_of(facts_ref, GIVEN_AS + j * len(spans), spans) for j in range(blocks)]
    out_ref[...] = jnp.transpose(jnp.concatenate(given, axis=0)).astype(bf16)


def body(states_in, span_order, pre_gain, w_query, w_key, w_value, w_out, post_gain):
    _, row_count, part = states_in.shape
    width = pre_gain.shape[1]
    q_width = w_query.shape[2]
    kv_width = w_key.shape[2]
    sections = lax.axis_size("section")
    tensors = lax.axis_size("tensor")
    seqs = lax.axis_size("seq")
    section_rank = lax.axis_index("section")
    seq_rank = lax.axis_index("seq")
    tensor_rank = lax.axis_index("tensor")
    spans = span_order.shape[0]
    rows = row_count // CHUNKS
    own = rows // tensors
    assert own == OWN
    chunk_len = rows * seqs
    block = (own * width // LANES, LANES)

    key_value = lambda tick: pl.pallas_call(
        functools.partial(key_value_kernel, tick),
        out_shape=(
            jax.ShapeDtypeStruct((rows, 2 * kv_width), bf16),
            jax.ShapeDtypeStruct((rows, width), bf16),
        ),
        in_specs=[VMEM] * 7,
        out_specs=(VMEM, VMEM),
        compiler_params=limit(10),
        name="key_value",
    )
    query = lambda tick: pl.pallas_call(
        functools.partial(query_kernel, tick),
        out_shape=jax.ShapeDtypeStruct((rows, q_width), bf16),
        in_specs=[VMEM] * 5,
        out_specs=VMEM,
        compiler_params=limit(8),
        name="query",
    )
    attention = lambda tick: pl.pallas_call(
        functools.partial(attention_kernel, tick),
        out_shape=jax.ShapeDtypeStruct((tensors, *block), bf16),
        in_specs=[VMEM] * 7,
        out_specs=VMEM,
        scratch_shapes=[pltpu.VMEM((rows, q_width), bf16)],
        compiler_params=limit(10),
        name="attention",
    )
    combine = pl.pallas_call(
        combine_kernel,
        out_shape=jax.ShapeDtypeStruct(block, bf16),
        in_specs=[VMEM, VMEM, VMEM],
        out_specs=VMEM,
        scratch_shapes=[pltpu.VMEM(block, f32)],
        compiler_params=limit(4),
        name="combine",
    )

    tick_total = sections + CHUNKS - 1
    half_spans = spans // seqs
    twin_first = jnp.concatenate([span_order[half_spans:], span_order[:half_spans]])
    near_first = jnp.where(seq_rank == 0, span_order, twin_first)
    ids = jnp.arange(spans, dtype=jnp.int32)
    rows_of_facts = [near_first == chunk * seqs + seq_rank for chunk in range(CHUNKS)]
    rows_of_facts += [(near_first[:half_spans, None] == ids[None, :]).reshape(-1)]
    rows_of_facts += [jnp.stack([section_rank, seq_rank, tensor_rank])]
    facts = jnp.concatenate([r.astype(f32) for r in rows_of_facts])
    facts = jnp.pad(facts, (0, FACTS - facts.shape[0]))
    facts = jnp.broadcast_to(facts[:, None], (FACTS, LANES))
    places = (
        jnp.arange(CHUNKS, dtype=jnp.int32)[:, None] * chunk_len
        + seq_rank * rows
        + jnp.arange(rows, dtype=jnp.int32)[None, :]
    )
    half = HEAD_DIM // 2
    inverse = rotary_base ** (-(jnp.arange(half, dtype=f32) * 2.0 / HEAD_DIM))
    angles = places.astype(f32)[..., None] * inverse
    cos_part, sin_part = jnp.cos(angles), jnp.sin(angles)
    cos_full = jnp.concatenate([cos_part, cos_part], axis=-1)
    sin_full = jnp.concatenate([-sin_part, sin_part], axis=-1)

    mine = jnp.transpose(states_in[0])
    theirs = lax.ppermute(mine, "seq", [(0, 1), (1, 0)])
    sent = (rows + own) * (part // LANES) + FOLD * own
    pieces = pl.pallas_call(
        pick_kernel,
        out_shape=jax.ShapeDtypeStruct((tensors, sent, LANES), bf16),
        in_specs=[VMEM, VMEM, VMEM],
        out_specs=VMEM,
        compiler_params=limit(4),
        name="pick",
    )(facts, mine, theirs)
    no_past = jnp.zeros((rows, 2 * kv_width), bf16)
    pieces, facts, cos_full, sin_full, no_past = lax.optimization_barrier(
        (pieces, facts, cos_full, sin_full, no_past)
    )
    full, held, following = pl.pallas_call(
        gather_kernel,
        out_shape=(
            jax.ShapeDtypeStruct((tensors, *block), bf16),
            jax.ShapeDtypeStruct(block, bf16),
            jax.ShapeDtypeStruct(block, bf16),
        ),
        in_specs=[VMEM, VMEM],
        out_specs=(VMEM, VMEM, VMEM),
        scratch_shapes=[pltpu.VMEM((rows + own, width), f32)],
        compiler_params=limit(6),
        name="gather",
    )(facts, exchange(pieces, "tensor"))

    past = (no_past, no_past)
    made = []
    for tick in range(tick_total):
        kv_own, normed = key_value(tick)(facts, full, pre_gain, cos_full, sin_full, w_key, w_value)
        kv_other = lax.ppermute(kv_own, "seq", [(0, 1), (1, 0)])
        queries = query(tick)(facts, normed, cos_full, sin_full, w_query)
        terms = attention(tick)(facts, queries, kv_own, kv_other, *past, w_out)
        past = (kv_own, kv_other)
        made.append(combine(exchange(terms, "tensor"), held, post_gain))
        if tick + 1 < tick_total:
            busy = [i for i in range(sections - 1) if 0 <= tick - i < CHUNKS]
            held = lax.ppermute(made[-1], "section", [(i, i + 1) for i in busy])
            if tick + 1 < CHUNKS:
                held = pl.pallas_call(
                    choose_kernel,
                    out_shape=jax.ShapeDtypeStruct(block, bf16),
                    in_specs=[VMEM] * 3,
                    out_specs=VMEM,
                    compiler_params=limit(2),
                    name="choose",
                )(facts, held, following)
            full = exchange(jnp.broadcast_to(held[None], (tensors, *block)), "tensor")

    made = lax.optimization_barrier(tuple(made))
    pieces = pl.pallas_call(
        split_kernel,
        out_shape=jax.ShapeDtypeStruct((seqs, tensors, CHUNKS, own, part), bf16),
        in_specs=[VMEM] * (tick_total + 1),
        out_specs=VMEM,
        scratch_shapes=[pltpu.VMEM((own, width), f32)],
        compiler_params=limit(6),
        name="split",
    )(facts, *made)
    pieces = exchange(pieces.reshape(seqs * tensors, CHUNKS, own, part), ("seq", "tensor"))
    out = pl.pallas_call(
        order_kernel,
        out_shape=jax.ShapeDtypeStruct((part, row_count), bf16),
        in_specs=[VMEM, VMEM],
        out_specs=VMEM,
        compiler_params=limit(4),
        name="order",
    )(facts, pieces.reshape(seqs, tensors, CHUNKS, own, part))
    return jnp.transpose(out)[None, None]


def solution(mesh):
    in_specs = (
        P(None, "seq", "tensor"),
        P(),
        P("section", None),
        P("section", None, "tensor"),
        P("section", None, "tensor"),
        P("section", None, "tensor"),
        P("section", "tensor", None),
        P("section", None),
    )
    out_specs = P("section", None, "seq", "tensor")
    return jax.shard_map(body, mesh=mesh, in_specs=in_specs, out_specs=out_specs, check_vma=False)
```

```python
import functools

import jax
import jax.numpy as jnp
from jax import lax
from jax.experimental import pallas as pl
from jax.experimental.pallas import tpu as pltpu
from jax.sharding import PartitionSpec as P

HEAD_DIM = 128
CHUNKS = 2
LANES = 128
OWN = 8
OUT_STEPS = 3
FOLD = 5

softcap_limit = 50.0
query_scale = 144.0 ** (-0.5)
epsilon = 1e-06
rotary_base = 10000.0
f32 = jnp.float32
bf16 = jnp.bfloat16

VMEM = pl.BlockSpec(memory_space=pltpu.VMEM)

FIRST_FROM, SECOND_FROM, GIVEN_AS = 0, 4, 8
SECTION, CORE, OWNER, FACTS = 16, 17, 18, 24
MIB = 1024 * 1024


def limit(mib):
    return pltpu.CompilerParams(vmem_limit_bytes=mib * MIB)


def exchange(pieces, axes):
    return lax.all_to_all(pieces, axes, split_axis=0, concat_axis=0, tiled=True)


def tiles(ref_shape):
    return range(ref_shape[-2] // OWN)


def tile(c):
    return slice(c * OWN, (c + 1) * OWN)


def fact(facts_ref, row):
    return facts_ref[row:row + 1, :]


def one_of(facts_ref, first, choices):
    picked = choices[0]
    for i in range(1, len(choices)):
        picked = jnp.where(facts_ref[first + i:first + i + 1, :1] > 0, choices[i], picked)
    return picked


def is_later(facts_ref, tick):
    return fact(facts_ref, SECTION) <= tick - 1


def lanes(c):
    return slice(c * LANES, (c + 1) * LANES)


def rope(u, cos_full, sin_full):
    return u * cos_full + pltpu.roll(u, HEAD_DIM // 2, 1) * sin_full


def key_value_kernel(tick, facts_ref, x_ref, gain_ref, cos_ref, sin_ref, wk_ref, wv_ref,
                     kv_ref, normed_ref):
    rows, width = normed_ref.shape
    kv_width = wk_ref.shape[2]
    squares = jnp.zeros((rows, LANES), f32)
    for c in tiles(x_ref.shape):
        x = x_ref[:, tile(c)].astype(f32).reshape(rows, LANES)
        squares += x * x
    scaling = lax.rsqrt(jnp.sum(squares, axis=1, keepdims=True) / width + epsilon)
    for c in tiles(x_ref.shape):
        x = x_ref[:, tile(c)].astype(f32).reshape(rows, LANES)
        normed_ref[:, lanes(c)] = (x * scaling * gain_ref[:, lanes(c)].astype(f32)).astype(bf16)
    later = is_later(facts_ref, tick)
    cos_full = jnp.where(later, cos_ref[1], cos_ref[0])
    sin_full = jnp.where(later, sin_ref[1], sin_ref[0])
    keys = jnp.dot(normed_ref[...], wk_ref[0], preferred_element_type=f32)
    for head in range(kv_width // HEAD_DIM):
        at = slice(head * HEAD_DIM, (head + 1) * HEAD_DIM)
        kv_ref[:, at] = rope(keys[:, at], cos_full, sin_full).astype(bf16)
    values = jnp.dot(normed_ref[...], wv_ref[0], preferred_element_type=f32)
    kv_ref[:, kv_width:] = values.astype(bf16)


def early_kernel(tick, facts_ref, normed_ref, cos_ref, sin_ref, wq_ref, own_ref,
                 past_own_ref, past_other_ref, wo_ref, out_ref, q_ref, attended_ref):
    @pl.when(jnp.max(fact(facts_ref, CORE)) < 1)
    def _():
        query_part(tick, facts_ref, normed_ref, cos_ref, sin_ref, wq_ref, q_ref)
        attention_part(
            tick, facts_ref, q_ref, own_ref, own_ref, past_own_ref, past_other_ref, wo_ref,
            out_ref, attended_ref,
        )


def late_query_kernel(tick, facts_ref, normed_ref, cos_ref, sin_ref, wq_ref, q_ref):
    @pl.when(jnp.max(fact(facts_ref, CORE)) > 0)
    def _():
        query_part(tick, facts_ref, normed_ref, cos_ref, sin_ref, wq_ref, q_ref)


def late_kernel(tick, facts_ref, q_ref, own_ref, other_ref, past_own_ref, past_other_ref, wo_ref,
                done_ref, out_ref, attended_ref):
    is_late = jnp.max(fact(facts_ref, CORE)) > 0

    @pl.when(is_late)
    def _():
        attention_part(
            tick, facts_ref, q_ref, own_ref, other_ref, past_own_ref, past_other_ref, wo_ref,
            out_ref, attended_ref,
        )

    @pl.when(jnp.logical_not(is_late))
    def _():
        out_ref[...] = done_ref[...]


def query_part(tick, facts_ref, normed_ref, cos_ref, sin_ref, wq_ref, q_ref):
    q_width = q_ref.shape[1]
    later = is_later(facts_ref, tick)
    cos_full = jnp.where(later, cos_ref[1], cos_ref[0])
    sin_full = jnp.where(later, sin_ref[1], sin_ref[0])
    pair = 2 * HEAD_DIM

    @pl.loop(0, q_width // pair)
    def _(p):
        at = pl.ds(pl.multiple_of(p * pair, pair), pair)
        queries = jnp.dot(normed_ref[...], wq_ref[0, :, at], preferred_element_type=f32)
        turned = [rope(queries[:, lanes(h)], cos_full, sin_full) * query_scale for h in range(2)]
        q_ref[:, at] = jnp.concatenate(turned, axis=1).astype(bf16)


def attention_part(tick, facts_ref, q_ref, own_ref, other_ref, past_own_ref, past_other_ref, wo_ref,
                   out_ref, attended_ref):
    rows, q_width = q_ref.shape
    kv_width = own_ref.shape[1] // 2
    kv_heads = kv_width // HEAD_DIM
    group = q_width // kv_width
    sources = (own_ref, other_ref, past_own_ref, past_other_ref)
    half = 2 * rows
    row = lax.broadcasted_iota(jnp.int32, (group * rows, half), 0) % rows
    col = lax.broadcasted_iota(jnp.int32, (group * rows, half), 1)
    after = jnp.broadcast_to(fact(facts_ref, CORE) > 0, (group * rows, half))
    has_past = jnp.broadcast_to(is_later(facts_ref, tick), (group * rows, half))
    now = ((col < rows) & (col <= row)) | ((col >= rows) & after)
    for head in range(kv_heads):
        at = slice(head * HEAD_DIM, (head + 1) * HEAD_DIM)
        value_at = slice(kv_width + head * HEAD_DIM, kv_width + (head + 1) * HEAD_DIM)
        keys = jnp.concatenate([s[:, at] for s in sources], axis=0)
        values = jnp.concatenate([s[:, value_at] for s in sources], axis=0)
        first = head * group * HEAD_DIM
        queries = jnp.concatenate(
            [q_ref[:, first + g * HEAD_DIM:first + (g + 1) * HEAD_DIM] for g in range(group)], axis=0
        )
        scores = lax.dot_general(
            queries, keys, (((1,), (1,)), ((), ())), preferred_element_type=f32
        )
        capped = softcap_limit * jnp.tanh(scores / softcap_limit)
        weight = jnp.exp(capped)
        weight = jnp.concatenate(
            [
                jnp.where(now, weight[:, :half], f32(0.0)),
                jnp.where(has_past, weight[:, half:], f32(0.0)),
            ],
            axis=1,
        )
        totals = jnp.sum(weight, axis=1, keepdims=True)
        numerator = jnp.dot(weight.astype(bf16), values, preferred_element_type=f32)
        attended = (numerator / totals).astype(bf16)
        for g in range(group):
            attended_ref[:, first + g * HEAD_DIM:first + (g + 1) * HEAD_DIM] = attended[
                g * rows:(g + 1) * rows
            ]
    count = out_ref.shape[1] // OWN // OUT_STEPS

    @pl.loop(0, OUT_STEPS)
    def _(n):
        at = pl.ds(pl.multiple_of(n * count * LANES, LANES), count * LANES)
        terms = jnp.dot(attended_ref[...], wo_ref[0, :, at], preferred_element_type=f32)
        blocks = [terms[:, lanes(c)].reshape(-1, OWN, LANES).astype(bf16) for c in range(count)]
        to = pl.ds(pl.multiple_of(n * count * OWN, 2 * OWN), count * OWN)
        out_ref[:, to] = jnp.concatenate(blocks, axis=1)


def combine_kernel(arrived_ref, held_ref, gain_ref, out_ref, sum_ref):
    width = gain_ref.shape[1]
    squares = jnp.zeros((OWN, LANES), f32)
    for c in tiles(out_ref.shape):
        projected = jnp.sum(arrived_ref[:, tile(c)].astype(f32), axis=0)
        sum_ref[tile(c)] = projected
        squares += projected * projected
    scaling = lax.rsqrt(jnp.sum(squares, axis=1, keepdims=True) / width + epsilon)
    for c in tiles(out_ref.shape):
        scaled = sum_ref[tile(c)] * scaling * gain_ref[:, lanes(c)].astype(f32)
        out_ref[tile(c)] = (held_ref[tile(c)].astype(f32) + scaled).astype(bf16)


def choose_kernel(facts_ref, moved_ref, following_ref, held_ref):
    is_first = fact(facts_ref, SECTION) < 1
    moved, following = moved_ref[...].astype(f32), following_ref[...].astype(f32)
    held_ref[...] = jnp.where(is_first, following, moved).astype(bf16)


def pick_kernel(facts_ref, mine_ref, theirs_ref, out_ref):
    peers = out_ref.shape[0]
    both = [jnp.transpose(ref[...].astype(f32)) for ref in (mine_ref, theirs_ref)]
    rows = both[0].shape[0] // CHUNKS
    part = both[0].shape[1]
    blocks = [b[i * rows:(i + 1) * rows] for b in both for i in range(CHUNKS)]
    first = one_of(facts_ref, FIRST_FROM, blocks)
    second = one_of(facts_ref, SECOND_FROM, blocks)
    sent, whole = rows + OWN, part // LANES
    kept = FOLD * OWN
    for t in range(peers):
        own = second[t * OWN:(t + 1) * OWN]
        for c in range(whole):
            out_ref[t, c * sent:c * sent + rows] = first[:, lanes(c)].astype(bf16)
            out_ref[t, c * sent + rows:(c + 1) * sent] = own[:, lanes(c)].astype(bf16)
        rest = slice(whole * LANES, part)
        upper = jnp.concatenate([first[kept:, rest], own[:, rest], own[:, rest]], axis=0)
        fold = jnp.concatenate([first[:kept, rest], upper], axis=1)
        out_ref[t, whole * sent:] = fold.astype(bf16)


def gather_kernel(facts_ref, arrived_ref, full_ref, held_ref, next_ref, flat_ref):
    peers = full_ref.shape[0]
    rows = peers * OWN
    part = flat_ref.shape[1] // peers
    sent, whole = rows + OWN, part // LANES
    kept = FOLD * OWN
    rest = part - whole * LANES
    for t in range(peers):
        for c in range(whole):
            piece = arrived_ref[t, c * sent:(c + 1) * sent].astype(f32)
            flat_ref[:, t * part + c * LANES:t * part + (c + 1) * LANES] = piece
        fold = arrived_ref[t, whole * sent:].astype(f32)
        at = slice((t + 1) * part - rest, (t + 1) * part)
        flat_ref[:kept, at] = fold[:, :rest]
        flat_ref[kept:, at] = fold[:sent - kept, rest:]
    owner = fact(facts_ref, OWNER)
    for c in tiles(next_ref.shape):
        blocks = flat_ref[:rows, lanes(c)].reshape(peers, OWN, LANES)
        full_ref[:, tile(c)] = blocks.astype(bf16)
        held = blocks[0]
        for t in range(1, peers):
            held = jnp.where(owner == t, blocks[t], held)
        held_ref[tile(c)] = held.astype(bf16)
        next_ref[tile(c)] = flat_ref[rows:, lanes(c)].astype(bf16)


def split_kernel(facts_ref, *refs):
    *made_refs, out_ref, flat_ref = refs
    cores, peers, chunks, _, part = out_ref.shape
    section = fact(facts_ref, SECTION)
    for chunk in range(chunks):
        rows = made_refs[chunk][...].astype(f32)
        for i in range(1, len(made_refs) - chunks + 1):
            rows = jnp.where(section == i, made_refs[i + chunk][...].astype(f32), rows)
        for c in tiles(rows.shape):
            flat_ref[:, lanes(c)] = rows[tile(c)]
        for t in range(peers):
            piece = flat_ref[:, t * part:(t + 1) * part].astype(bf16)
            for core in range(cores):
                out_ref[core, t, chunk] = piece


def order_kernel(facts_ref, arrived_ref, out_ref):
    cores, peers, chunks, _, part = arrived_ref.shape
    rows = peers * OWN
    spans = [
        arrived_ref[core, :, chunk].astype(f32).reshape(rows, part)
        for chunk in range(chunks)
        for core in reversed(range(cores))
    ]
    blocks = out_ref.shape[1] // rows
    given = [one_of(facts_ref, GIVEN_AS + j * len(spans), spans) for j in range(blocks)]
    out_ref[...] = jnp.transpose(jnp.concatenate(given, axis=0)).astype(bf16)


def body(states_in, span_order, pre_gain, w_query, w_key, w_value, w_out, post_gain):
    _, row_count, part = states_in.shape
    width = pre_gain.shape[1]
    q_width = w_query.shape[2]
    kv_width = w_key.shape[2]
    sections = lax.axis_size("section")
    tensors = lax.axis_size("tensor")
    seqs = lax.axis_size("seq")
    section_rank = lax.axis_index("section")
    seq_rank = lax.axis_index("seq")
    tensor_rank = lax.axis_index("tensor")
    spans = span_order.shape[0]
    place = seqs - 1 - seq_rank
    rows = row_count // CHUNKS
    own = rows // tensors
    assert own == OWN
    chunk_len = rows * seqs
    block = (own * width // LANES, LANES)

    key_value = lambda tick: pl.pallas_call(
        functools.partial(key_value_kernel, tick),
        out_shape=(
            jax.ShapeDtypeStruct((rows, 2 * kv_width), bf16),
            jax.ShapeDtypeStruct((rows, width), bf16),
        ),
        in_specs=[VMEM] * 7,
        out_specs=(VMEM, VMEM),
        compiler_params=limit(10),
        name="key_value",
    )

    terms_shape = jax.ShapeDtypeStruct((tensors, *block), bf16)
    q_shape = (rows, q_width)
    early = lambda tick: pl.pallas_call(
        functools.partial(early_kernel, tick),
        out_shape=terms_shape,
        in_specs=[VMEM] * 9,
        out_specs=VMEM,
        scratch_shapes=[pltpu.VMEM(q_shape, bf16)] * 2,
        compiler_params=limit(16),
        name="early",
    )
    late_query = lambda tick: pl.pallas_call(
        functools.partial(late_query_kernel, tick),
        out_shape=jax.ShapeDtypeStruct(q_shape, bf16),
        in_specs=[VMEM] * 5,
        out_specs=VMEM,
        compiler_params=limit(8),
        name="late_query",
    )
    late = lambda tick: pl.pallas_call(
        functools.partial(late_kernel, tick),
        out_shape=terms_shape,
        in_specs=[VMEM] * 8,
        out_specs=VMEM,
        scratch_shapes=[pltpu.VMEM(q_shape, bf16)],
        compiler_params=limit(12),
        name="late",
    )
    combine = pl.pallas_call(
        combine_kernel,
        out_shape=jax.ShapeDtypeStruct(block, bf16),
        in_specs=[VMEM, VMEM, VMEM],
        out_specs=VMEM,
        scratch_shapes=[pltpu.VMEM(block, f32)],
        compiler_params=limit(4),
        name="combine",
    )

    tick_total = sections + CHUNKS - 1
    half_spans = spans // seqs
    twin_first = jnp.concatenate([span_order[half_spans:], span_order[:half_spans]])
    near_first = jnp.where(seq_rank == 0, span_order, twin_first)
    ids = jnp.arange(spans, dtype=jnp.int32)
    rows_of_facts = [near_first == chunk * seqs + place for chunk in range(CHUNKS)]
    rows_of_facts += [(near_first[:half_spans, None] == ids[None, :]).reshape(-1)]
    rows_of_facts += [jnp.stack([section_rank, place, tensor_rank])]
    facts = jnp.concatenate([r.astype(f32) for r in rows_of_facts])
    facts = jnp.pad(facts, (0, FACTS - facts.shape[0]))
    facts = jnp.broadcast_to(facts[:, None], (FACTS, LANES))
    places = (
        jnp.arange(CHUNKS, dtype=jnp.int32)[:, None] * chunk_len
        + place * rows
        + jnp.arange(rows, dtype=jnp.int32)[None, :]
    )
    half = HEAD_DIM // 2
    inverse = rotary_base ** (-(jnp.arange(half, dtype=f32) * 2.0 / HEAD_DIM))
    angles = places.astype(f32)[..., None] * inverse
    cos_part, sin_part = jnp.cos(angles), jnp.sin(angles)
    cos_full = jnp.concatenate([cos_part, cos_part], axis=-1)
    sin_full = jnp.concatenate([-sin_part, sin_part], axis=-1)

    mine = jnp.transpose(states_in[0])
    theirs = lax.ppermute(mine, "seq", [(0, 1), (1, 0)])
    sent = (rows + own) * (part // LANES) + FOLD * own
    pieces = pl.pallas_call(
        pick_kernel,
        out_shape=jax.ShapeDtypeStruct((tensors, sent, LANES), bf16),
        in_specs=[VMEM, VMEM, VMEM],
        out_specs=VMEM,
        compiler_params=limit(4),
        name="pick",
    )(facts, mine, theirs)
    no_past = jnp.zeros((rows, 2 * kv_width), bf16)
    pieces, facts, cos_full, sin_full, no_past = lax.optimization_barrier(
        (pieces, facts, cos_full, sin_full, no_past)
    )
    full, held, following = pl.pallas_call(
        gather_kernel,
        out_shape=(
            jax.ShapeDtypeStruct((tensors, *block), bf16),
            jax.ShapeDtypeStruct(block, bf16),
            jax.ShapeDtypeStruct(block, bf16),
        ),
        in_specs=[VMEM, VMEM],
        out_specs=(VMEM, VMEM, VMEM),
        scratch_shapes=[pltpu.VMEM((rows + own, width), f32)],
        compiler_params=limit(6),
        name="gather",
    )(facts, exchange(pieces, "tensor"))

    past = (no_past, no_past)
    made = []
    for tick in range(tick_total):
        kv_own, normed = key_value(tick)(facts, full, pre_gain, cos_full, sin_full, w_key, w_value)
        terms = early(tick)(facts, normed, cos_full, sin_full, w_query, kv_own, *past, w_out)
        kv_own, normed, terms = lax.optimization_barrier((kv_own, normed, terms))
        kv_other = lax.ppermute(kv_own, "seq", [(0, 1), (1, 0)])
        queries = late_query(tick)(facts, normed, cos_full, sin_full, w_query)
        terms = late(tick)(facts, queries, kv_own, kv_other, *past, w_out, terms)
        past = (kv_own, kv_other)
        made.append(combine(exchange(terms, "tensor"), held, post_gain))
        if tick + 1 < tick_total:
            busy = [i for i in range(sections - 1) if 0 <= tick - i < CHUNKS]
            held = lax.ppermute(made[-1], "section", [(i, i + 1) for i in busy])
            if tick + 1 < CHUNKS:
                held = pl.pallas_call(
                    choose_kernel,
                    out_shape=jax.ShapeDtypeStruct(block, bf16),
                    in_specs=[VMEM] * 3,
                    out_specs=VMEM,
                    compiler_params=limit(2),
                    name="choose",
                )(facts, held, following)
            full = exchange(jnp.broadcast_to(held[None], (tensors, *block)), "tensor")

    made = lax.optimization_barrier(tuple(made))
    pieces = pl.pallas_call(
        split_kernel,
        out_shape=jax.ShapeDtypeStruct((seqs, tensors, CHUNKS, own, part), bf16),
        in_specs=[VMEM] * (tick_total + 1),
        out_specs=VMEM,
        scratch_shapes=[pltpu.VMEM((own, width), f32)],
        compiler_params=limit(6),
        name="split",
    )(facts, *made)
    pieces = exchange(pieces.reshape(seqs * tensors, CHUNKS, own, part), ("seq", "tensor"))
    out = pl.pallas_call(
        order_kernel,
        out_shape=jax.ShapeDtypeStruct((part, row_count), bf16),
        in_specs=[VMEM, VMEM],
        out_specs=VMEM,
        compiler_params=limit(4),
        name="order",
    )(facts, pieces.reshape(seqs, tensors, CHUNKS, own, part))
    return jnp.transpose(out)[None, None]


def solution(mesh):
    in_specs = (
        P(None, "seq", "tensor"),
        P(),
        P("section", None),
        P("section", None, "tensor"),
        P("section", None, "tensor"),
        P("section", None, "tensor"),
        P("section", "tensor", None),
        P("section", None),
    )
    out_specs = P("section", None, "seq", "tensor")
    return jax.shard_map(body, mesh=mesh, in_specs=in_specs, out_specs=out_specs, check_vma=False)
```

```python
import functools

import jax
import jax.numpy as jnp
from jax import lax
from jax.experimental import pallas as pl
from jax.experimental.pallas import tpu as pltpu
from jax.sharding import PartitionSpec as P

HEAD_DIM = 128
CHUNKS = 2
LANES = 128
OWN = 8
OUT_STEPS = 3
FOLD = 5

softcap_limit = 50.0
query_scale = 144.0 ** (-0.5)
epsilon = 1e-06
rotary_base = 10000.0
f32 = jnp.float32
bf16 = jnp.bfloat16

VMEM = pl.BlockSpec(memory_space=pltpu.VMEM)

FIRST_FROM, SECOND_FROM, GIVEN_AS = 0, 4, 8
SECTION, CORE, OWNER, FACTS = 16, 17, 18, 24
MIB = 1024 * 1024


def limit(mib):
    return pltpu.CompilerParams(vmem_limit_bytes=mib * MIB)


def exchange(pieces, axes):
    return lax.all_to_all(pieces, axes, split_axis=0, concat_axis=0, tiled=True)


def tiles(ref_shape):
    return range(ref_shape[-2] // OWN)


def tile(c):
    return slice(c * OWN, (c + 1) * OWN)


def fact(facts_ref, row):
    return facts_ref[row:row + 1, :]


def one_of(facts_ref, first, choices):
    picked = choices[0]
    for i in range(1, len(choices)):
        picked = jnp.where(facts_ref[first + i:first + i + 1, :1] > 0, choices[i], picked)
    return picked


def is_later(facts_ref, tick):
    return fact(facts_ref, SECTION) <= tick - 1


def lanes(c):
    return slice(c * LANES, (c + 1) * LANES)


def rope(u, cos_full, sin_full):
    return u * cos_full + pltpu.roll(u, HEAD_DIM // 2, 1) * sin_full


def key_value_kernel(tick, facts_ref, x_ref, gain_ref, cos_ref, sin_ref, wk_ref, wv_ref,
                     kv_ref, normed_ref):
    rows, width = normed_ref.shape
    kv_width = wk_ref.shape[2]
    squares = jnp.zeros((rows, LANES), f32)
    for c in tiles(x_ref.shape):
        x = x_ref[:, tile(c)].astype(f32).reshape(rows, LANES)
        squares += x * x
    scaling = lax.rsqrt(jnp.sum(squares, axis=1, keepdims=True) / width + epsilon)
    for c in tiles(x_ref.shape):
        x = x_ref[:, tile(c)].astype(f32).reshape(rows, LANES)
        normed_ref[:, lanes(c)] = (x * scaling * gain_ref[:, lanes(c)].astype(f32)).astype(bf16)
    later = is_later(facts_ref, tick)
    cos_full = jnp.where(later, cos_ref[1], cos_ref[0])
    sin_full = jnp.where(later, sin_ref[1], sin_ref[0])
    keys = jnp.dot(normed_ref[...], wk_ref[0], preferred_element_type=f32)
    for head in range(kv_width // HEAD_DIM):
        at = slice(head * HEAD_DIM, (head + 1) * HEAD_DIM)
        kv_ref[:, at] = rope(keys[:, at], cos_full, sin_full).astype(bf16)
    values = jnp.dot(normed_ref[...], wv_ref[0], preferred_element_type=f32)
    kv_ref[:, kv_width:] = values.astype(bf16)


def early_kernel(tick, facts_ref, normed_ref, cos_ref, sin_ref, wq_ref, own_ref,
                 past_own_ref, past_other_ref, wo_ref, out_ref, q_ref, attended_ref):
    @pl.when(jnp.max(fact(facts_ref, CORE)) < 1)
    def _():
        query_part(tick, facts_ref, normed_ref, cos_ref, sin_ref, wq_ref, q_ref)
        attention_part(
            tick, facts_ref, q_ref, own_ref, own_ref, past_own_ref, past_other_ref, wo_ref,
            out_ref, attended_ref,
        )


def late_query_kernel(tick, facts_ref, normed_ref, cos_ref, sin_ref, wq_ref, q_ref):
    @pl.when(jnp.max(fact(facts_ref, CORE)) > 0)
    def _():
        query_part(tick, facts_ref, normed_ref, cos_ref, sin_ref, wq_ref, q_ref)


def late_kernel(tick, facts_ref, q_ref, own_ref, other_ref, past_own_ref, past_other_ref, wo_ref,
                done_ref, out_ref, attended_ref):
    is_late = jnp.max(fact(facts_ref, CORE)) > 0

    @pl.when(is_late)
    def _():
        attention_part(
            tick, facts_ref, q_ref, own_ref, other_ref, past_own_ref, past_other_ref, wo_ref,
            out_ref, attended_ref,
        )

    @pl.when(jnp.logical_not(is_late))
    def _():
        out_ref[...] = done_ref[...]


def query_part(tick, facts_ref, normed_ref, cos_ref, sin_ref, wq_ref, q_ref):
    q_width = q_ref.shape[1]
    later = is_later(facts_ref, tick)
    cos_full = jnp.where(later, cos_ref[1], cos_ref[0])
    sin_full = jnp.where(later, sin_ref[1], sin_ref[0])
    pair = 2 * HEAD_DIM

    @pl.loop(0, q_width // pair)
    def _(p):
        at = pl.ds(pl.multiple_of(p * pair, pair), pair)
        queries = jnp.dot(normed_ref[...], wq_ref[0, :, at], preferred_element_type=f32)
        turned = [rope(queries[:, lanes(h)], cos_full, sin_full) * query_scale for h in range(2)]
        q_ref[:, at] = jnp.concatenate(turned, axis=1).astype(bf16)


def attention_part(tick, facts_ref, q_ref, own_ref, other_ref, past_own_ref, past_other_ref, wo_ref,
                   out_ref, attended_ref):
    rows, q_width = q_ref.shape
    kv_width = own_ref.shape[1] // 2
    kv_heads = kv_width // HEAD_DIM
    group = q_width // kv_width
    sources = (own_ref, other_ref, past_own_ref, past_other_ref)
    half = 2 * rows
    row = lax.broadcasted_iota(jnp.int32, (group * rows, half), 0) % rows
    col = lax.broadcasted_iota(jnp.int32, (group * rows, half), 1)
    after = jnp.broadcast_to(fact(facts_ref, CORE) > 0, (group * rows, half))
    has_past = jnp.broadcast_to(is_later(facts_ref, tick), (group * rows, half))
    now = ((col < rows) & (col <= row)) | ((col >= rows) & after)
    for head in range(kv_heads):
        at = slice(head * HEAD_DIM, (head + 1) * HEAD_DIM)
        value_at = slice(kv_width + head * HEAD_DIM, kv_width + (head + 1) * HEAD_DIM)
        keys = jnp.concatenate([s[:, at] for s in sources], axis=0)
        values = jnp.concatenate([s[:, value_at] for s in sources], axis=0)
        first = head * group * HEAD_DIM
        queries = jnp.concatenate(
            [q_ref[:, first + g * HEAD_DIM:first + (g + 1) * HEAD_DIM] for g in range(group)], axis=0
        )
        scores = lax.dot_general(
            queries, keys, (((1,), (1,)), ((), ())), preferred_element_type=f32
        )
        capped = softcap_limit * jnp.tanh(scores / softcap_limit)
        weight = jnp.exp(capped)
        weight = jnp.concatenate(
            [
                jnp.where(now, weight[:, :half], f32(0.0)),
                jnp.where(has_past, weight[:, half:], f32(0.0)),
            ],
            axis=1,
        )
        totals = jnp.sum(weight, axis=1, keepdims=True)
        numerator = jnp.dot(weight.astype(bf16), values, preferred_element_type=f32)
        attended = (numerator / totals).astype(bf16)
        for g in range(group):
            attended_ref[:, first + g * HEAD_DIM:first + (g + 1) * HEAD_DIM] = attended[
                g * rows:(g + 1) * rows
            ]
    count = out_ref.shape[1] // OWN // OUT_STEPS

    @pl.loop(0, OUT_STEPS)
    def _(n):
        at = pl.ds(pl.multiple_of(n * count * LANES, LANES), count * LANES)
        terms = jnp.dot(attended_ref[...], wo_ref[0, :, at], preferred_element_type=f32)
        blocks = [terms[:, lanes(c)].reshape(-1, OWN, LANES).astype(bf16) for c in range(count)]
        to = pl.ds(pl.multiple_of(n * count * OWN, 2 * OWN), count * OWN)
        out_ref[:, to] = jnp.concatenate(blocks, axis=1)


def combine_kernel(arrived_ref, held_ref, gain_ref, out_ref, sum_ref):
    width = gain_ref.shape[1]
    squares = jnp.zeros((OWN, LANES), f32)
    for c in tiles(out_ref.shape):
        projected = jnp.sum(arrived_ref[:, tile(c)].astype(f32), axis=0)
        sum_ref[tile(c)] = projected
        squares += projected * projected
    scaling = lax.rsqrt(jnp.sum(squares, axis=1, keepdims=True) / width + epsilon)
    for c in tiles(out_ref.shape):
        scaled = sum_ref[tile(c)] * scaling * gain_ref[:, lanes(c)].astype(f32)
        out_ref[tile(c)] = (held_ref[tile(c)].astype(f32) + scaled).astype(bf16)


def choose_kernel(facts_ref, moved_ref, following_ref, held_ref):
    is_first = fact(facts_ref, SECTION) < 1
    moved, following = moved_ref[...].astype(f32), following_ref[...].astype(f32)
    held_ref[...] = jnp.where(is_first, following, moved).astype(bf16)


def pick_kernel(facts_ref, mine_ref, theirs_ref, out_ref):
    peers = out_ref.shape[0]
    both = [jnp.transpose(ref[...].astype(f32)) for ref in (mine_ref, theirs_ref)]
    rows = both[0].shape[0] // CHUNKS
    part = both[0].shape[1]
    blocks = [b[i * rows:(i + 1) * rows] for b in both for i in range(CHUNKS)]
    first = one_of(facts_ref, FIRST_FROM, blocks)
    second = one_of(facts_ref, SECOND_FROM, blocks)
    sent, whole = rows + OWN, part // LANES
    kept = FOLD * OWN
    for t in range(peers):
        own = second[t * OWN:(t + 1) * OWN]
        for c in range(whole):
            out_ref[t, c * sent:c * sent + rows] = first[:, lanes(c)].astype(bf16)
            out_ref[t, c * sent + rows:(c + 1) * sent] = own[:, lanes(c)].astype(bf16)
        rest = slice(whole * LANES, part)
        upper = jnp.concatenate([first[kept:, rest], own[:, rest], own[:, rest]], axis=0)
        fold = jnp.concatenate([first[:kept, rest], upper], axis=1)
        out_ref[t, whole * sent:] = fold.astype(bf16)


def gather_kernel(facts_ref, arrived_ref, *refs):
    full_ref, held_ref, next_ref, flat_ref = refs[-4:]
    peers = full_ref.shape[0]
    rows = peers * OWN
    part = flat_ref.shape[1] // peers
    sent, whole = rows + OWN, part // LANES
    kept = FOLD * OWN
    rest = part - whole * LANES
    for t in range(peers):
        for c in range(whole):
            piece = arrived_ref[t, c * sent:(c + 1) * sent].astype(f32)
            flat_ref[:, t * part + c * LANES:t * part + (c + 1) * LANES] = piece
        fold = arrived_ref[t, whole * sent:].astype(f32)
        at = slice((t + 1) * part - rest, (t + 1) * part)
        flat_ref[:kept, at] = fold[:, :rest]
        flat_ref[kept:, at] = fold[:sent - kept, rest:]
    owner = fact(facts_ref, OWNER)
    for c in tiles(next_ref.shape):
        blocks = flat_ref[:rows, lanes(c)].reshape(peers, OWN, LANES)
        full_ref[:, tile(c)] = blocks.astype(bf16)
        held = blocks[0]
        for t in range(1, peers):
            held = jnp.where(owner == t, blocks[t], held)
        held_ref[tile(c)] = held.astype(bf16)
        next_ref[tile(c)] = flat_ref[rows:, lanes(c)].astype(bf16)


def split_kernel(facts_ref, *refs):
    *made_refs, out_ref, flat_ref = refs
    cores, peers, chunks, _, part = out_ref.shape
    section = fact(facts_ref, SECTION)
    for chunk in range(chunks):
        rows = made_refs[chunk][...].astype(f32)
        for i in range(1, len(made_refs) - chunks + 1):
            rows = jnp.where(section == i, made_refs[i + chunk][...].astype(f32), rows)
        for c in tiles(rows.shape):
            flat_ref[:, lanes(c)] = rows[tile(c)]
        for t in range(peers):
            piece = flat_ref[:, t * part:(t + 1) * part].astype(bf16)
            for core in range(cores):
                out_ref[core, t, chunk] = piece


def order_kernel(facts_ref, arrived_ref, out_ref):
    cores, peers, chunks, _, part = arrived_ref.shape
    rows = peers * OWN
    spans = [
        arrived_ref[core, :, chunk].astype(f32).reshape(rows, part)
        for chunk in range(chunks)
        for core in reversed(range(cores))
    ]
    blocks = out_ref.shape[1] // rows
    given = [one_of(facts_ref, GIVEN_AS + j * len(spans), spans) for j in range(blocks)]
    out_ref[...] = jnp.transpose(jnp.concatenate(given, axis=0)).astype(bf16)


def body(states_in, span_order, pre_gain, w_query, w_key, w_value, w_out, post_gain):
    _, row_count, part = states_in.shape
    width = pre_gain.shape[1]
    q_width = w_query.shape[2]
    kv_width = w_key.shape[2]
    sections = lax.axis_size("section")
    tensors = lax.axis_size("tensor")
    seqs = lax.axis_size("seq")
    section_rank = lax.axis_index("section")
    seq_rank = lax.axis_index("seq")
    tensor_rank = lax.axis_index("tensor")
    spans = span_order.shape[0]
    place = seqs - 1 - seq_rank
    rows = row_count // CHUNKS
    own = rows // tensors
    assert own == OWN
    chunk_len = rows * seqs
    block = (own * width // LANES, LANES)

    key_value = lambda tick: pl.pallas_call(
        functools.partial(key_value_kernel, tick),
        out_shape=(
            jax.ShapeDtypeStruct((rows, 2 * kv_width), bf16),
            jax.ShapeDtypeStruct((rows, width), bf16),
        ),
        in_specs=[VMEM] * 7,
        out_specs=(VMEM, VMEM),
        compiler_params=limit(10),
        name="key_value",
    )

    terms_shape = jax.ShapeDtypeStruct((tensors, *block), bf16)
    q_shape = (rows, q_width)
    early = lambda tick: pl.pallas_call(
        functools.partial(early_kernel, tick),
        out_shape=terms_shape,
        in_specs=[VMEM] * 9,
        out_specs=VMEM,
        scratch_shapes=[pltpu.VMEM(q_shape, bf16)] * 2,
        compiler_params=limit(16),
        name="early",
    )
    late_query = lambda tick: pl.pallas_call(
        functools.partial(late_query_kernel, tick),
        out_shape=jax.ShapeDtypeStruct(q_shape, bf16),
        in_specs=[VMEM] * 5,
        out_specs=VMEM,
        compiler_params=limit(8),
        name="late_query",
    )
    late = lambda tick: pl.pallas_call(
        functools.partial(late_kernel, tick),
        out_shape=terms_shape,
        in_specs=[VMEM] * 8,
        out_specs=VMEM,
        scratch_shapes=[pltpu.VMEM(q_shape, bf16)],
        compiler_params=limit(12),
        name="late",
    )
    combine = pl.pallas_call(
        combine_kernel,
        out_shape=jax.ShapeDtypeStruct(block, bf16),
        in_specs=[VMEM, VMEM, VMEM],
        out_specs=VMEM,
        scratch_shapes=[pltpu.VMEM(block, f32)],
        compiler_params=limit(4),
        name="combine",
    )

    tick_total = sections + CHUNKS - 1
    half_spans = spans // seqs
    twin_first = jnp.concatenate([span_order[half_spans:], span_order[:half_spans]])
    near_first = jnp.where(seq_rank == 0, span_order, twin_first)
    ids = jnp.arange(spans, dtype=jnp.int32)
    rows_of_facts = [near_first == chunk * seqs + place for chunk in range(CHUNKS)]
    rows_of_facts += [(near_first[:half_spans, None] == ids[None, :]).reshape(-1)]
    rows_of_facts += [jnp.stack([section_rank, place, tensor_rank])]
    facts = jnp.concatenate([r.astype(f32) for r in rows_of_facts])
    facts = jnp.pad(facts, (0, FACTS - facts.shape[0]))
    facts = jnp.broadcast_to(facts[:, None], (FACTS, LANES))
    places = (
        jnp.arange(CHUNKS, dtype=jnp.int32)[:, None] * chunk_len
        + place * rows
        + jnp.arange(rows, dtype=jnp.int32)[None, :]
    )
    half = HEAD_DIM // 2
    inverse = rotary_base ** (-(jnp.arange(half, dtype=f32) * 2.0 / HEAD_DIM))
    angles = places.astype(f32)[..., None] * inverse
    cos_part, sin_part = jnp.cos(angles), jnp.sin(angles)
    cos_full = jnp.concatenate([cos_part, cos_part], axis=-1)
    sin_full = jnp.concatenate([-sin_part, sin_part], axis=-1)

    mine = jnp.transpose(states_in[0])
    theirs = lax.ppermute(mine, "seq", [(0, 1), (1, 0)])
    sent = (rows + own) * (part // LANES) + FOLD * own
    pieces = pl.pallas_call(
        pick_kernel,
        out_shape=jax.ShapeDtypeStruct((tensors, sent, LANES), bf16),
        in_specs=[VMEM, VMEM, VMEM],
        out_specs=VMEM,
        compiler_params=limit(4),
        name="pick",
    )(facts, mine, theirs)
    no_past = jnp.zeros((rows, 2 * kv_width), bf16)
    pieces, facts, cos_full, sin_full, no_past = lax.optimization_barrier(
        (pieces, facts, cos_full, sin_full, no_past)
    )
    full, held, following = pl.pallas_call(
        gather_kernel,
        out_shape=(
            jax.ShapeDtypeStruct((tensors, *block), bf16),
            jax.ShapeDtypeStruct(block, bf16),
            jax.ShapeDtypeStruct(block, bf16),
        ),
        in_specs=[VMEM] * 5,
        out_specs=(VMEM, VMEM, VMEM),
        scratch_shapes=[pltpu.VMEM((rows + own, width), f32)],
        compiler_params=limit(16),
        name="gather",
    )(facts, exchange(pieces, "tensor"), w_value, pre_gain, w_out)

    past = (no_past, no_past)
    made = []
    for tick in range(tick_total):
        kv_own, normed = key_value(tick)(facts, full, pre_gain, cos_full, sin_full, w_key, w_value)
        terms = early(tick)(facts, normed, cos_full, sin_full, w_query, kv_own, *past, w_out)
        kv_own, normed, terms = lax.optimization_barrier((kv_own, normed, terms))
        kv_other = lax.ppermute(kv_own, "seq", [(0, 1), (1, 0)])
        queries = late_query(tick)(facts, normed, cos_full, sin_full, w_query)
        terms = late(tick)(facts, queries, kv_own, kv_other, *past, w_out, terms)
        past = (kv_own, kv_other)
        made.append(combine(exchange(terms, "tensor"), held, post_gain))
        if tick + 1 < tick_total:
            busy = [i for i in range(sections - 1) if 0 <= tick - i < CHUNKS]
            held = lax.ppermute(made[-1], "section", [(i, i + 1) for i in busy])
            if tick + 1 < CHUNKS:
                held = pl.pallas_call(
                    choose_kernel,
                    out_shape=jax.ShapeDtypeStruct(block, bf16),
                    in_specs=[VMEM] * 3,
                    out_specs=VMEM,
                    compiler_params=limit(2),
                    name="choose",
                )(facts, held, following)
            full = exchange(jnp.broadcast_to(held[None], (tensors, *block)), "tensor")

    made = lax.optimization_barrier(tuple(made))
    pieces = pl.pallas_call(
        split_kernel,
        out_shape=jax.ShapeDtypeStruct((seqs, tensors, CHUNKS, own, part), bf16),
        in_specs=[VMEM] * (tick_total + 1),
        out_specs=VMEM,
        scratch_shapes=[pltpu.VMEM((own, width), f32)],
        compiler_params=limit(6),
        name="split",
    )(facts, *made)
    pieces = exchange(pieces.reshape(seqs * tensors, CHUNKS, own, part), ("seq", "tensor"))
    out = pl.pallas_call(
        order_kernel,
        out_shape=jax.ShapeDtypeStruct((part, row_count), bf16),
        in_specs=[VMEM, VMEM],
        out_specs=VMEM,
        compiler_params=limit(4),
        name="order",
    )(facts, pieces.reshape(seqs, tensors, CHUNKS, own, part))
    return jnp.transpose(out)[None, None]


def solution(mesh):
    in_specs = (
        P(None, "seq", "tensor"),
        P(),
        P("section", None),
        P("section", None, "tensor"),
        P("section", None, "tensor"),
        P("section", None, "tensor"),
        P("section", "tensor", None),
        P("section", None),
    )
    out_specs = P("section", None, "seq", "tensor")
    return jax.shard_map(body, mesh=mesh, in_specs=in_specs, out_specs=out_specs, check_vma=False)
```
